32 devices in a mesh: groups: 2 (over y), curve: 16 (over z, x, core).
Axes of the slice: x: 2, y: 2, z: 4, core: 2. Of those that a mesh axis runs over, the one named last changes fastest.
Arguments:
- tracer_mass: float32 [9216, 200], P(('groups', 'curve')), parts along dimension 0, may hold values from 0.1 to 10
- send_ids: int32 [128, 32], P(('groups', 'curve')), parts along dimension 0, may hold values from 0 to 31, as said below
- send_counts: int32 [128], P(('groups', 'curve')), parts along dimension 0, may hold values from 1 to 32, as said below
- sources: int32 [9216, 4], P(('groups', 'curve')), parts along dimension 0, may hold values from 0 to 1439
- fractions: float32 [9216, 4], P(('groups', 'curve')), parts along dimension 0, may hold values from 0.02 to 0.25
- moments: float32 [2, 9216, 4], P(None, ('groups', 'curve')), parts along dimension 1, may hold values from -0.5 to 0.5
Outputs:
- new_mass: float32 [9216, 200], P(('groups', 'curve')), parts along dimension 0
The draws below stay inside these ranges and needn't reach their ends.
There are 2 independent parts, one for each index of `groups`. The reference program is written for one: setup_inputs(seed, part) draws one part's arguments, and reference() takes and returns one part's arrays. A program takes and returns all parts, laid end to end along the dimension named above; each array names one. Nothing has to cross between parts.
Inputs may be any that keep to these rules, and one draw needn't show every extreme that they name: `send_ids`: each row holds distinct local element indices of the owning device. `send_counts`: slots below the count are live; in every draw some lists reach 32. `sources`: indices into the device's own extended cells.
All inputs are finite; a program needn't handle non-finite values.
Results may differ from the reference program's by a relative error of at most 0.0001.
Values sent between devices are 32-bit elements; how exact they have to be, the bound alone decides.
No kernel may reach another device: no remote copies, remote signals or barrier semaphores. Data moves between devices by JAX's collectives and lax.ppermute only.
A program may use at most 64 MiB of HBM per device.

```python
import math
import jax
import jax.numpy as jnp
from jax import lax

E_DEV = 32
SEND = 32
PIECES = 4
LT = 200
LISTS = 64
CELLS_ALL = 4608
EXT_CELLS = 1440
N_CURVE = 16


def draw_send_ids(key, part):
    scores = jax.random.randint(jax.random.fold_in(key, 11), (LISTS, E_DEV), 0, 2 ** 20) * E_DEV + jnp.arange(E_DEV, dtype=jnp.int32)[None, :]
    order = jnp.argsort(scores, axis=1, stable=True)
    return order[:, :SEND].astype(jnp.int32)


def draw_send_counts(key, part):
    counts = jax.random.randint(jax.random.fold_in(key, 23), (LISTS,), max(1, SEND // 8), SEND + 1)
    forced = jnp.arange(LISTS, dtype=jnp.int32) % 5 == 0
    return jnp.where(forced, SEND, counts).astype(jnp.int32)


def place_ends(entries, key, low, largest):
    extent = entries.shape
    spot = [jax.random.randint(jax.random.fold_in(key, axis), (), 0, extent[axis]) for axis in range(len(extent))]
    entries = entries.at[tuple(spot)].set(low)
    longest = extent.index(max(extent))
    spot[longest] = (spot[longest] + 1) % extent[longest]
    return entries.at[tuple(spot)].set(largest)


def level_of(rng, shape, split, smallest, high):
    loudness = 1.0
    for position, parts in split:
        steps = jax.random.uniform(jax.random.fold_in(jax.random.fold_in(rng, 6), position), (parts,), jnp.float32, smallest / len(split), high / len(split))
        loudness = loudness * jnp.repeat(jnp.exp(steps), shape[position] // parts).reshape((-1,) + (1,) * (len(shape) - 1 - position))
    return loudness


def setup_inputs(seed: int = 0, part: int = 0) -> dict:
    arg_keys = jax.random.split(jax.random.key(seed), 7)
    part_keys = jax.random.split(jax.random.fold_in(arg_keys[6], part), 7)
    tracer_mass = jnp.clip(jnp.exp(math.log(10.0) - 4.6051702 * jax.random.uniform(part_keys[0], (CELLS_ALL, LT), jnp.float32) ** level_of(part_keys[0], (CELLS_ALL, LT), ((0, 16),), -0.2, 0.2)), 0.1, 10.0)
    send_ids = draw_send_ids(jax.random.fold_in(jax.random.fold_in(arg_keys[6], part), 71), part)
    send_counts = draw_send_counts(jax.random.fold_in(jax.random.fold_in(arg_keys[6], part), 71), part)
    sources = place_ends(jax.random.randint(part_keys[3], (CELLS_ALL, PIECES), 0, EXT_CELLS), jax.random.fold_in(part_keys[3], 1), 0, EXT_CELLS - 1).astype(jnp.int32)
    fractions = jnp.clip(0.02 + 0.23 * jax.random.uniform(part_keys[4], (CELLS_ALL, PIECES), jnp.float32) ** level_of(part_keys[4], (CELLS_ALL, PIECES), ((0, 16),), -0.2, 0.2), 0.02, 0.25)
    moments = jnp.clip(jax.random.uniform(part_keys[5], (2, CELLS_ALL, PIECES), jnp.float32, -0.5, 0.5) * level_of(part_keys[5], (2, CELLS_ALL, PIECES), ((1, 16),), -0.4, 0.0), -0.5, 0.5)
    return dict(tracer_mass=tracer_mass, send_ids=send_ids, send_counts=send_counts, sources=sources, fractions=fractions, moments=moments)


OFFSETS = (1, 2, -1, -2)


def differ(cells, axis):
    first = jnp.take(cells, 0, axis=axis)
    middle = jnp.take(cells, 1, axis=axis)
    last = jnp.take(cells, 2, axis=axis)
    return jnp.stack([middle - first, 0.5 * (last - first), last - middle], axis=axis)


def transport(extended, sources_dev, fraction_dev, moment_x, moment_y):
    width = extended.shape[-1]
    total_cells = extended.shape[0] * 9
    cells = extended.reshape(-1, 3, 3, width)
    slope_x = differ(cells, 2).reshape(-1, 9, width)
    slope_y = differ(cells, 1).reshape(-1, 9, width)
    table = jnp.stack([extended, slope_x, slope_y], axis=2).reshape(total_cells, 3, width)
    inflow = jnp.zeros((sources_dev.shape[0], width), jnp.float32)
    outflow = jnp.zeros((total_cells, width), jnp.float32)
    for column in range(sources_dev.shape[1]):
        picked = table[sources_dev[:, column]]
        flux = fraction_dev[:, column, None] * (picked[:, 0] + moment_x[:, column, None] * picked[:, 1] + moment_y[:, column, None] * picked[:, 2])
        inflow = inflow + flux
        outflow = outflow + jax.ops.segment_sum(flux, sources_dev[:, column], num_segments=total_cells)
    return inflow, outflow


def reference(tracer_mass, send_ids, send_counts, sources, fractions, moments):
    mass = tracer_mass.reshape(N_CURVE, E_DEV, 9, LT)
    id_lists = send_ids.reshape(N_CURVE, 4, SEND).astype(jnp.int32)
    counts = send_counts.reshape(N_CURVE, 4)
    live = (jnp.arange(SEND, dtype=jnp.int32)[None, None, :] < counts[:, :, None]).astype(jnp.float32)
    packed = jax.vmap(lambda block, idx: block[idx])(mass, id_lists) * live[..., None, None]
    received = jnp.stack([jnp.roll(packed[:, slot], OFFSETS[slot], axis=0) for slot in range(4)], axis=1)
    extended = jnp.concatenate([mass, received.reshape(N_CURVE, 4 * SEND, 9, LT)], axis=1)
    src_all = sources.reshape(N_CURVE, 9 * E_DEV, PIECES).astype(jnp.int32)
    frac_all = fractions.reshape(N_CURVE, 9 * E_DEV, PIECES)
    mom_x = moments[0].reshape(N_CURVE, 9 * E_DEV, PIECES)
    mom_y = moments[1].reshape(N_CURVE, 9 * E_DEV, PIECES)

    def per_device(items):
        return transport(*items)

    inflow, outflow = lax.map(per_device, (extended, src_all, frac_all, mom_x, mom_y))
    returned = outflow[:, 9 * E_DEV:].reshape(N_CURVE, 4, SEND, 9, LT)
    back = jnp.stack([jnp.roll(returned[:, slot], -OFFSETS[slot], axis=0) for slot in range(4)], axis=1)
    back = back * live[..., None, None]
    own = outflow[:, :9 * E_DEV].reshape(N_CURVE, E_DEV, 9, LT)
    own = jax.vmap(lambda block, idx, extra: block.at[idx.reshape(-1)].add(extra.reshape(-1, 9, LT)))(own, id_lists, back)
    result = mass + inflow.reshape(N_CURVE, E_DEV, 9, LT) - own
    return result.reshape(CELLS_ALL, LT)
```

```python
import functools

import jax
import jax.numpy as jnp
from jax import lax
from jax.experimental import pallas as pl
from jax.experimental.pallas import tpu as pltpu
from jax.sharding import PartitionSpec as P

LANES = 128
F32 = jnp.float32
BF16 = jnp.bfloat16


def round8(n):
    return -(-n // 8) * 8


class Plan:
    def __init__(self, cells, width, elements, slots):
        self.cells, self.width, self.elements, self.slots = cells, width, elements, slots
        self.full = width // LANES
        rest = width % LANES
        self.rest = rest
        self.parts = []
        row = self.full * cells
        lane, size = 0, LANES // 2
        while rest:
            if rest >= size:
                groups = LANES // size
                height = round8(-(-cells // groups))
                self.parts.append((lane, size, height, row))
                row += height
                lane += size
                rest -= size
            size //= 2
        self.table = row
        self.rows = row + slots
        self.group = LANES // 4
        self.tiles = self.full + (1 if self.parts else 0)

    def pack(self, tile_rows, out):
        cells = self.cells
        for t in range(self.full):
            out[t * cells:(t + 1) * cells, :] = tile_rows(t)
        if not self.parts:
            return
        last = tile_rows(self.full)
        for lane, size, height, first in self.parts:
            lanes = lax.broadcasted_iota(jnp.int32, (height, LANES), 1)
            total = None
            for g in range(-(-cells // height)):
                count = min(height, cells - g * height)
                piece = last[g * height:g * height + count]
                shift = (g * size - lane) % LANES
                if shift:
                    piece = pltpu.roll(piece, shift, 1)
                if count < height:
                    piece = jnp.concatenate([piece, jnp.zeros((height - count, LANES), F32)], axis=0)
                total = piece if total is None else jnp.where(lanes >= g * size, piece, total)
            out[first:first + height, :] = total

    def unpack(self, ref):
        cells = self.cells
        tiles = [ref[t * cells:(t + 1) * cells, :] for t in range(self.full)]
        if self.parts:
            last = None
            for lane, size, height, first in self.parts:
                block = ref[first:first + height, :]
                pieces = []
                for g in range(-(-cells // height)):
                    shift = (lane - g * size) % LANES
                    piece = pltpu.roll(block, shift, 1) if shift else block
                    pieces.append(piece[:min(height, cells - g * height)])
                piece = jnp.concatenate(pieces, axis=0)
                lanes = lax.broadcasted_iota(jnp.int32, (cells, LANES), 1)
                last = piece if last is None else jnp.where(lanes >= lane, piece, last)
            tiles.append(last)
        return tiles


def split(x):
    high = x.astype(BF16)
    return high, (x - high.astype(F32)).astype(BF16)


def dot(a, b):
    return jnp.dot(a, b, preferred_element_type=F32)


def element_and_place(src):
    elem = ((src.astype(F32) + 0.5) * (1.0 / 9.0)).astype(jnp.int32)
    return elem, src - 9 * elem


def pack_kernel(plan, q_ref, src_ref, fr_ref, mo_ref, ids_ref, cnt_ref, out_ref, own_ref, t_ref):
    cells, E, S = plan.cells, plan.elements, plan.slots
    for t in range(plan.full):
        t_ref[t] = q_ref[:, t * LANES:(t + 1) * LANES]
    if plan.rest:
        t_ref[plan.full, :, 0:plan.rest] = q_ref[:, plan.full * LANES:plan.width]

    def tile_rows(t):
        return jnp.concatenate([t_ref[t, pl.ds(p, E, stride=9), :] for p in range(9)], axis=0)

    plan.pack(tile_rows, out_ref)
    elem, place = element_and_place(src_ref[...])
    fr = fr_ref[...]
    wx = fr * mo_ref[0]
    wy = fr * mo_ref[1]
    total = E + 4 * S
    erow = lax.broadcasted_iota(jnp.int32, (total, cells), 0)
    urow = lax.broadcasted_iota(jnp.int32, (32, cells), 0)
    uplace = urow - jnp.where(urow < 9, 0, jnp.where(urow < 18, 9, 18))
    acc = None
    for k in range(src_ref.shape[0]):
        hot = jnp.where(erow == elem[k:k + 1, :], 1.0, 0.0).astype(BF16)
        value = jnp.where(urow < 9, fr[k:k + 1, :], jnp.where(urow < 18, wx[k:k + 1, :], wy[k:k + 1, :]))
        value = jnp.where(uplace == place[k:k + 1, :], value, 0.0)
        high, low = split(value)
        both = jnp.concatenate([high, low, jnp.zeros((64, cells), BF16)], axis=0)
        got = lax.dot_general(hot, both, (((1,), (1,)), ((), ())), preferred_element_type=F32)
        acc = got if acc is None else acc + got
    acc = acc + pltpu.roll(acc, LANES - 32, 1)
    own_ref[...] = acc[0:E]
    lane = lax.broadcasted_iota(jnp.int32, (S, LANES), 1)
    table = jnp.zeros((S, LANES), F32)
    diag = lax.broadcasted_iota(jnp.int32, (S, S), 0) == lax.broadcasted_iota(jnp.int32, (S, S), 1)
    slot = lax.broadcasted_iota(jnp.int32, (1, S), 1)
    for o in range(4):
        part = acc[E + o * S:E + (o + 1) * S]
        if o:
            part = pltpu.roll(part, plan.group * o, 1)
        inside = (lane >= plan.group * o) & (lane < plan.group * o + 27)
        table = jnp.where(inside, part, table)
        ids = jnp.where(slot < cnt_ref[o], ids_ref[o:o + 1, :].astype(F32), -1.0)
        column = jnp.sum(jnp.where(diag, ids, 0.0), axis=1, keepdims=True)
        table = jnp.where(lane == plan.group * o + 27, column, table)
    out_ref[plan.table:plan.table + S, :] = table


def matrix_kernel(plan, src_ref, fr_ref, mo_ref, hi_ref, lo_ref, col_ref):
    cells, E = plan.cells, plan.elements
    K = src_ref.shape[0]
    elem, place = element_and_place(src_ref[...])
    fr = fr_ref[...]
    wx = fr * mo_ref[0]
    wy = fr * mo_ref[1]
    row = jnp.where(place >= 6, 2, jnp.where(place >= 3, 1, 0))
    r = row.astype(F32)
    c = (place - 3 * row).astype(F32)
    centre = fr + wx * (c - 1.0) + wy * (r - 1.0)
    rows = [
        elem.astype(F32), place.astype(F32), centre,
        wx * (1.0 - 0.5 * c), wx * (-0.5 * c), wy * (1.0 - 0.5 * r), wy * (-0.5 * r),
    ]
    rows = jnp.concatenate(rows + [jnp.zeros((LANES - 7 * K, cells), F32)], axis=0)
    pad = -cells % LANES
    if pad:
        rows = jnp.concatenate([rows, jnp.zeros((LANES, pad), F32)], axis=1)
    col_ref[...] = jnp.transpose(rows, (1, 0))[0:cells]
    step = E
    lane = lax.broadcasted_iota(jnp.int32, (step, LANES), 1)
    per = LANES // E
    lists = hi_ref.shape[0]

    def body(i, carry):
        at = pl.multiple_of(i * step, step)
        cols = col_ref[pl.ds(at, step), :]

        def wide(n, k):
            return jnp.broadcast_to(cols[:, n * K + k:n * K + k + 1], (step, LANES))

        for t in range(-(-9 // per)):
            where = (lane // E + per * t).astype(F32)
            inner = (lane % E).astype(F32)
            sums = [jnp.zeros((step, LANES), F32) for _ in range(lists)]
            for k in range(K):
                d = where - wide(1, k)
                coef = jnp.where(d == 0.0, wide(2, k), 0.0)
                coef = jnp.where(d == 1.0, wide(3, k), coef)
                coef = jnp.where(d == -1.0, wide(4, k), coef)
                coef = jnp.where(d == 3.0, wide(5, k), coef)
                coef = jnp.where(d == -3.0, wide(6, k), coef)
                e = wide(0, k) - inner
                for n in range(lists):
                    sums[n] = sums[n] + jnp.where(e == float(n * E), coef, 0.0)
            size = min(LANES, 9 * E - t * LANES)
            for n in range(lists):
                high, low = split(sums[n])
                hi_ref[n, pl.ds(at, step), t * LANES:t * LANES + size] = high[:, :size]
                lo_ref[n, pl.ds(at, step), t * LANES:t * LANES + size] = low[:, :size]
        return carry

    lax.fori_loop(0, cells // step, body, 0)


def apply_block(plan, tiles, ids, hi, lo):
    E, S = plan.elements, plan.slots
    masses = jnp.concatenate(tiles, axis=1)
    high, low = split(masses)
    if ids is not None:
        per = LANES // E
        r = lax.broadcasted_iota(jnp.int32, (LANES, LANES), 0)
        l = lax.broadcasted_iota(jnp.int32, (LANES, LANES), 1)
        many = jnp.concatenate([ids] * per, axis=0)
        hot = jnp.where(((l % E).astype(F32) == many) & (r // E == l // E), 1.0, 0.0).astype(BF16)
        pair = jnp.concatenate([high, low], axis=1)
        pieces = []
        for first in range(0, plan.cells, LANES):
            size = min(LANES, plan.cells - first)
            pieces.append(dot(hot[:size, :size], pair[first:first + size]).astype(BF16))
        pair = jnp.concatenate(pieces, axis=0)
        high, low = pair[:, :masses.shape[1]], pair[:, masses.shape[1]:]
    return dot(hi, high) + dot(hi, low) + dot(lo, high)


def table_ids(plan, table, which):
    lane = lax.broadcasted_iota(jnp.int32, table.shape, 1)
    return jnp.sum(jnp.where(lane == plan.group * which + 27, table, 0.0), axis=1, keepdims=True)


def returned_weights(plan, table, which, ids_ref, cnt_ref):
    E, S = plan.elements, plan.slots
    part = pltpu.roll(table, lax.rem(LANES - plan.group * which, LANES), 1)
    lane = lax.broadcasted_iota(jnp.int32, (S, LANES), 1)
    part = jnp.where(lane < 27, part, 0.0)
    high, low = split(part)
    slot = lax.broadcasted_iota(jnp.int32, (E, S), 1)
    e = lax.broadcasted_iota(jnp.int32, (E, S), 0)
    live = (e == ids_ref[pl.ds(which, 1), :]) & (slot < cnt_ref[which])
    hot = jnp.where(live, 1.0, 0.0).astype(BF16)
    return dot(hot, high) + dot(hot, low)


def kept(plan, tiles, weights, out_ref):
    E = plan.elements
    for p in range(9):
        w = [jnp.broadcast_to(weights[:, 9 * j + p:9 * j + p + 1], (E, LANES)) for j in range(3)]
        for t in range(plan.tiles):
            def at(i):
                return tiles[t][i * E:(i + 1) * E]

            def slope(pos, step):
                if pos == 0:
                    return at(p + step) - at(p)
                if pos == 1:
                    return 0.5 * (at(p + step) - at(p - step))
                return at(p) - at(p - step)

            value = at(p) - (w[0] * at(p) + w[1] * slope(p % 3, 1) + w[2] * slope(p // 3, 3))
            out_ref[t, pl.ds(p, E, stride=9), :] = value


def final_kernel(plan, ids_ref, cnt_ref, own_w_ref, own_ref, x_ref, s_ref, y_ref, f_ref,
                 hi_ref, lo_ref, out_ref, t_ref):
    S = plan.slots
    odd = lax.rem(lax.axis_index("curve"), 2)
    tiles = plan.unpack(own_ref)
    inflow = apply_block(plan, tiles, None, hi_ref[0], lo_ref[0])
    weights = own_w_ref[...]
    for ref, even_list, odd_list in ((s_ref, 0, 2), (x_ref, 1, 3), (f_ref, 2, 0), (y_ref, 3, 1)):
        mine = jnp.where(odd == 1, odd_list, even_list)
        theirs = lax.rem(mine + 2, 4)
        table = ref[plan.table:plan.table + S, :]
        weights = weights + returned_weights(plan, table, mine, ids_ref, cnt_ref)
        ids = table_ids(plan, table, theirs)
        inflow = inflow + apply_block(plan, plan.unpack(ref), ids, hi_ref[theirs + 1], lo_ref[theirs + 1])
    kept(plan, tiles, weights, t_ref)
    for t in range(plan.full):
        out_ref[:, t * LANES:(t + 1) * LANES] = t_ref[t] + inflow[:, t * LANES:(t + 1) * LANES]
    if plan.rest:
        at = plan.full * LANES
        out_ref[:, at:plan.width] = (t_ref[plan.full] + inflow[:, at:at + LANES])[:, :plan.rest]


def send(x, table):
    return lax.ppermute(x, "curve", table)


def local(tracer_mass, send_ids, send_counts, sources, fractions, moments):
    count = lax.axis_size("curve")
    cells, width = tracer_mass.shape
    slots = send_ids.shape[1]
    elements = cells // 9
    plan = Plan(cells, width, elements, slots)
    src, fr, mo = sources.T, fractions.T, jnp.transpose(moments, (0, 2, 1))
    vmem = pl.BlockSpec(memory_space=pltpu.VMEM)
    smem = pl.BlockSpec(memory_space=pltpu.SMEM)
    payload, own_w = pl.pallas_call(
        functools.partial(pack_kernel, plan),
        out_shape=(
            jax.ShapeDtypeStruct((plan.rows, LANES), F32),
            jax.ShapeDtypeStruct((elements, LANES), F32),
        ),
        in_specs=[vmem] * 5 + [smem],
        out_specs=(vmem, vmem),
        scratch_shapes=[pltpu.VMEM((plan.tiles, cells, LANES), F32)],
        name="pack",
    )(tracer_mass, src, fr, mo, send_ids, send_counts)
    towards = [(i, (i + (2 if i % 2 else -2)) % count) for i in range(count)]
    away = [(i, (i - (2 if i % 2 else -2)) % count) for i in range(count)]
    swap = [(i, i ^ 1) for i in range(count)]
    got_x = send(payload, towards)
    got_s = send(payload, swap)
    got_y = send(payload, away)
    got_f = send(got_x, swap)
    hi, lo = pl.pallas_call(
        functools.partial(matrix_kernel, plan),
        out_shape=(jax.ShapeDtypeStruct((5, cells, cells), BF16),) * 2,
        in_specs=[vmem] * 3,
        out_specs=(vmem, vmem),
        scratch_shapes=[pltpu.VMEM((cells, LANES), F32)],
        cost_estimate=pl.CostEstimate(flops=2 * 10**9, bytes_accessed=2 * 10**6, transcendentals=0),
        name="matrix",
    )(src, fr, mo)
    return pl.pallas_call(
        functools.partial(final_kernel, plan),
        out_shape=jax.ShapeDtypeStruct((cells, width), F32),
        in_specs=[vmem, smem] + [vmem] * 8,
        out_specs=vmem,
        scratch_shapes=[pltpu.VMEM((plan.tiles, cells, LANES), F32)],
        name="final",
    )(send_ids, send_counts, own_w, payload, got_x, got_s, got_y, got_f, hi, lo)


def solution(mesh):
    placed = (
        P(("groups", "curve"), None),
        P(("groups", "curve"), None),
        P(("groups", "curve")),
        P(("groups", "curve"), None),
        P(("groups", "curve"), None),
        P(None, ("groups", "curve"), None),
    )
    return jax.shard_map(
        local, mesh=mesh, in_specs=placed, out_specs=P(("groups", "curve"), None), check_vma=False
    )
```

```python
import functools

import jax
import jax.numpy as jnp
from jax import lax
from jax.experimental import pallas as pl
from jax.experimental.pallas import tpu as pltpu
from jax.sharding import PartitionSpec as P


LANES = 128
F32 = jnp.float32
BF16 = jnp.bfloat16


def round8(n):
    return -(-n // 8) * 8


class Plan:
    def __init__(self, cells, width, elements, slots):
        self.cells, self.width, self.elements, self.slots = cells, width, elements, slots
        self.full = width // LANES
        rest = width % LANES
        self.rest = rest
        self.parts = []
        row = self.full * cells
        lane, size = 0, LANES // 2
        while rest:
            if rest >= size:
                groups = LANES // size
                height = round8(-(-cells // groups))
                self.parts.append((lane, size, height, row))
                row += height
                lane += size
                rest -= size
            size //= 2
        self.table = row
        self.rows = row + slots
        self.group = LANES // 4
        self.tiles = self.full + (1 if self.parts else 0)

    def pack(self, tile_rows, out):
        cells = self.cells
        for t in range(self.full):
            out[t * cells:(t + 1) * cells, :] = tile_rows(t)
        if not self.parts:
            return
        last = tile_rows(self.full)
        for lane, size, height, first in self.parts:
            lanes = lax.broadcasted_iota(jnp.int32, (height, LANES), 1)
            total = None
            for g in range(-(-cells // height)):
                count = min(height, cells - g * height)
                piece = last[g * height:g * height + count]
                shift = (g * size - lane) % LANES
                if shift:
                    piece = pltpu.roll(piece, shift, 1)
                if count < height:
                    piece = jnp.concatenate([piece, jnp.zeros((height - count, LANES), F32)], axis=0)
                total = piece if total is None else jnp.where(lanes >= g * size, piece, total)
            out[first:first + height, :] = total

    def unpack(self, ref):
        cells = self.cells
        tiles = [ref[t * cells:(t + 1) * cells, :] for t in range(self.full)]
        if self.parts:
            last = None
            for lane, size, height, first in self.parts:
                block = ref[first:first + height, :]
                pieces = []
                for g in range(-(-cells // height)):
                    shift = (lane - g * size) % LANES
                    piece = pltpu.roll(block, shift, 1) if shift else block
                    pieces.append(piece[:min(height, cells - g * height)])
                piece = jnp.concatenate(pieces, axis=0)
                lanes = lax.broadcasted_iota(jnp.int32, (cells, LANES), 1)
                last = piece if last is None else jnp.where(lanes >= lane, piece, last)
            tiles.append(last)
        return tiles


def split(x):
    high = x.astype(BF16)
    return high, (x - high.astype(F32)).astype(BF16)


def dot(a, b):
    return jnp.dot(a, b, preferred_element_type=F32)


def element_and_place(src):
    elem = ((src.astype(F32) + 0.5) * (1.0 / 9.0)).astype(jnp.int32)
    return elem, src - 9 * elem


def pack_kernel(plan, q_hbm, src_hbm, fr_hbm, mo_hbm, ids_hbm, cnt_hbm, out_ref, own_ref,
                src_ref, fr_ref, mo_ref, q_ref, ids_ref, cnt_ref, t_ref, sems):
    E = plan.elements
    copies = [
        pltpu.make_async_copy(a, b, sems.at[n])
        for n, (a, b) in enumerate((
            (src_hbm, src_ref), (fr_hbm, fr_ref), (mo_hbm, mo_ref),
            (cnt_hbm, cnt_ref), (ids_hbm, ids_ref), (q_hbm, q_ref),
        ))
    ]
    for copy in copies:
        copy.start()
    for copy in copies[:5]:
        copy.wait()
    weights_table(plan, src_ref, fr_ref, mo_ref, ids_ref, cnt_ref, out_ref, own_ref)
    copies[5].wait()
    for t in range(plan.full):
        t_ref[t] = q_ref[:, t * LANES:(t + 1) * LANES]
    if plan.rest:
        t_ref[plan.full, :, 0:plan.rest] = q_ref[:, plan.full * LANES:plan.width]

    def tile_rows(t):
        return jnp.concatenate([t_ref[t, pl.ds(p, E, stride=9), :] for p in range(9)], axis=0)

    plan.pack(tile_rows, out_ref)


def weights_table(plan, src_ref, fr_ref, mo_ref, ids_ref, cnt_ref, out_ref, own_ref):
    cells, E, S = plan.cells, plan.elements, plan.slots
    elem, place = element_and_place(src_ref[...])
    fr = fr_ref[...]
    wx = fr * mo_ref[0]
    wy = fr * mo_ref[1]
    total = E + 4 * S
    erow = lax.broadcasted_iota(jnp.int32, (total, cells), 0)
    urow = lax.broadcasted_iota(jnp.int32, (32, cells), 0)
    uplace = urow - jnp.where(urow < 9, 0, jnp.where(urow < 18, 9, 18))
    acc = None
    for k in range(src_ref.shape[0]):
        hot = jnp.where(erow == elem[k:k + 1, :], 1.0, 0.0).astype(BF16)
        value = jnp.where(urow < 9, fr[k:k + 1, :], jnp.where(urow < 18, wx[k:k + 1, :], wy[k:k + 1, :]))
        value = jnp.where(uplace == place[k:k + 1, :], value, 0.0)
        high, low = split(value)
        both = jnp.concatenate([high, low, jnp.zeros((64, cells), BF16)], axis=0)
        got = lax.dot_general(hot, both, (((1,), (1,)), ((), ())), preferred_element_type=F32)
        acc = got if acc is None else acc + got
    acc = acc + pltpu.roll(acc, LANES - 32, 1)
    own_ref[...] = acc[0:E]
    lane = lax.broadcasted_iota(jnp.int32, (S, LANES), 1)
    table = jnp.zeros((S, LANES), F32)
    diag = lax.broadcasted_iota(jnp.int32, (S, S), 0) == lax.broadcasted_iota(jnp.int32, (S, S), 1)
    slot = lax.broadcasted_iota(jnp.int32, (1, S), 1)
    for o in range(4):
        part = acc[E + o * S:E + (o + 1) * S]
        if o:
            part = pltpu.roll(part, plan.group * o, 1)
        inside = (lane >= plan.group * o) & (lane < plan.group * o + 27)
        table = jnp.where(inside, part, table)
        ids = jnp.where(slot < cnt_ref[o], ids_ref[o:o + 1, :].astype(F32), -1.0)
        column = jnp.sum(jnp.where(diag, ids, 0.0), axis=1, keepdims=True)
        table = jnp.where(lane == plan.group * o + 27, column, table)
    out_ref[plan.table:plan.table + S, :] = table


def matrix_kernel(plan, src_ref, fr_ref, mo_ref, hi_ref, lo_ref, col_ref):
    cells, E = plan.cells, plan.elements
    K = src_ref.shape[0]
    elem, place = element_and_place(src_ref[...])
    fr = fr_ref[...]
    wx = fr * mo_ref[0]
    wy = fr * mo_ref[1]
    row = jnp.where(place >= 6, 2, jnp.where(place >= 3, 1, 0))
    r = row.astype(F32)
    c = (place - 3 * row).astype(F32)
    centre = fr + wx * (c - 1.0) + wy * (r - 1.0)
    rows = [
        elem.astype(F32), place.astype(F32), centre,
        wx * (1.0 - 0.5 * c), wx * (-0.5 * c), wy * (1.0 - 0.5 * r), wy * (-0.5 * r),
    ]
    rows = jnp.concatenate(rows + [jnp.zeros((LANES - 7 * K, cells), F32)], axis=0)
    pad = -cells % LANES
    if pad:
        rows = jnp.concatenate([rows, jnp.zeros((LANES, pad), F32)], axis=1)
    col_ref[...] = jnp.transpose(rows, (1, 0))[0:cells]
    step = E
    lane = lax.broadcasted_iota(jnp.int32, (step, LANES), 1)
    per = LANES // E
    lists = hi_ref.shape[0]

    def body(i, carry):
        at = pl.multiple_of(i * step, step)
        cols = col_ref[pl.ds(at, step), :]

        def wide(n, k):
            return jnp.broadcast_to(cols[:, n * K + k:n * K + k + 1], (step, LANES))

        for t in range(-(-9 // per)):
            where = (lane // E + per * t).astype(F32)
            inner = (lane % E).astype(F32)
            sums = [jnp.zeros((step, LANES), F32) for _ in range(lists)]
            for k in range(K):
                d = where - wide(1, k)
                coef = jnp.where(d == 0.0, wide(2, k), 0.0)
                coef = jnp.where(d == 1.0, wide(3, k), coef)
                coef = jnp.where(d == -1.0, wide(4, k), coef)
                coef = jnp.where(d == 3.0, wide(5, k), coef)
                coef = jnp.where(d == -3.0, wide(6, k), coef)
                e = wide(0, k) - inner
                for n in range(lists):
                    sums[n] = sums[n] + jnp.where(e == float(n * E), coef, 0.0)
            size = min(LANES, 9 * E - t * LANES)
            for n in range(lists):
                high, low = split(sums[n])
                hi_ref[n, pl.ds(at, step), t * LANES:t * LANES + size] = high[:, :size]
                lo_ref[n, pl.ds(at, step), t * LANES:t * LANES + size] = low[:, :size]
        return carry

    lax.fori_loop(0, cells // step, body, 0)


def apply_block(plan, tiles, ids, hi, lo):
    E = plan.elements
    masses = jnp.concatenate(tiles, axis=1)
    high, low = split(masses)
    if ids is not None:
        per = LANES // E
        r = lax.broadcasted_iota(jnp.int32, (LANES, LANES), 0)
        l = lax.broadcasted_iota(jnp.int32, (LANES, LANES), 1)
        many = jnp.concatenate([ids] * per, axis=0)
        hot = jnp.where(((l % E).astype(F32) == many) & (r // E == l // E), 1.0, 0.0).astype(BF16)
        pair = jnp.concatenate([high, low], axis=1)
        pieces = []
        for first in range(0, plan.cells, LANES):
            size = min(LANES, plan.cells - first)
            pieces.append(dot(hot[:size, :size], pair[first:first + size]).astype(BF16))
        pair = jnp.concatenate(pieces, axis=0)
        high, low = pair[:, :masses.shape[1]], pair[:, masses.shape[1]:]
    return dot(hi, high) + dot(hi, low) + dot(lo, high)


def table_ids(plan, table, which):
    lane = lax.broadcasted_iota(jnp.int32, table.shape, 1)
    return jnp.sum(jnp.where(lane == plan.group * which + 27, table, 0.0), axis=1, keepdims=True)


def returned_weights(plan, table, which, hot):
    part = pltpu.roll(table, lax.rem(LANES - plan.group * which, LANES), 1)
    lane = lax.broadcasted_iota(jnp.int32, part.shape, 1)
    part = jnp.where(lane < 27, part, 0.0)
    high, low = split(part)
    return dot(hot, high) + dot(hot, low)


def live_slots(plan, which, ids_ref, cnt_ref):
    E, S = plan.elements, plan.slots
    slot = lax.broadcasted_iota(jnp.int32, (E, S), 1)
    e = lax.broadcasted_iota(jnp.int32, (E, S), 0)
    live = (e == ids_ref[pl.ds(which, 1), :]) & (slot < cnt_ref[which])
    return jnp.where(live, 1.0, 0.0).astype(BF16)


def my_list(name, count):
    index = lax.axis_index("curve")
    odd = lax.rem(index, 2) == 1
    end = (index == 0) | (index == count - 1)
    beside = (index == 1) | (index == count - 2)
    swap = jnp.where(odd, 2, 0)
    near = jnp.where(odd, 3, 1)
    far = jnp.where(odd, 1, 3)
    if name == "f":
        return jnp.where(odd, 0, 2)
    if name == "w":
        return jnp.where(end, far, jnp.where(beside, near, swap))
    if name == "x":
        return jnp.where(beside, swap, near)
    return jnp.where(end, swap, far)


def arrived(plan, mine, block, hot, hi_ref, lo_ref):
    theirs = lax.rem(mine + 2, 4)
    table = block[plan.table:plan.rows, :]
    weights = returned_weights(plan, table, mine, hot)
    ids = table_ids(plan, table, theirs)
    inflow = apply_block(plan, plan.unpack(block), ids, hi_ref[theirs + 1], lo_ref[theirs + 1])
    return inflow, weights


def kept(plan, tiles, weights, out_ref):
    E = plan.elements
    for p in range(9):
        w = [jnp.broadcast_to(weights[:, 9 * j + p:9 * j + p + 1], (E, LANES)) for j in range(3)]
        for t in range(plan.tiles):
            def at(i):
                return tiles[t][i * E:(i + 1) * E]

            def slope(pos, step):
                if pos == 0:
                    return at(p + step) - at(p)
                if pos == 1:
                    return 0.5 * (at(p + step) - at(p - step))
                return at(p) - at(p - step)

            value = at(p) - (w[0] * at(p) + w[1] * slope(p % 3, 1) + w[2] * slope(p // 3, 3))
            out_ref[t, pl.ds(p, E, stride=9), :] = value


def first_kernel(plan, count, ids_ref, cnt_ref, own_ref, hi_ref, lo_ref, acc_ref, hot_ref):
    for n, name in enumerate("wxyf"):
        hot_ref[n] = live_slots(plan, my_list(name, count), ids_ref, cnt_ref)
    acc_ref[...] = apply_block(plan, plan.unpack(own_ref), None, hi_ref[0], lo_ref[0])


def next_kernel(plan, count, names, in_acc_ref, in_w_ref, hot_ref, *refs):
    blocks, (hi_ref, lo_ref, acc_ref, w_ref) = refs[:len(names)], refs[len(names):]
    acc, weights = in_acc_ref[...], in_w_ref[...]
    for name, ref in zip(names, blocks):
        hot = hot_ref["wxyf".index(name)]
        more, extra = arrived(plan, my_list(name, count), ref, hot, hi_ref, lo_ref)
        acc, weights = acc + more, weights + extra
    acc_ref[...] = acc
    w_ref[...] = weights


def last_kernel(plan, count, name, acc_ref, in_w_ref, hot_ref, own_ref, ref, hi_ref, lo_ref, out_ref, t_ref):
    hot = hot_ref["wxyf".index(name)]
    more, weights = arrived(plan, my_list(name, count), ref, hot, hi_ref, lo_ref)
    inflow = acc_ref[...] + more
    kept(plan, plan.unpack(own_ref), in_w_ref[...] + weights, t_ref)
    for t in range(plan.full):
        out_ref[:, t * LANES:(t + 1) * LANES] = t_ref[t] + inflow[:, t * LANES:(t + 1) * LANES]
    if plan.rest:
        at = plan.full * LANES
        out_ref[:, at:plan.width] = (t_ref[plan.full] + inflow[:, at:at + LANES])[:, :plan.rest]


GRANT = pltpu.CompilerParams(vmem_limit_bytes=8 * 2**20)
VMEM = pl.BlockSpec(memory_space=pltpu.VMEM)
SMEM = pl.BlockSpec(memory_space=pltpu.SMEM)


HBM = pl.BlockSpec(memory_space=pltpu.HBM)


def far(*arrays):
    return [pltpu.with_memory_space_constraint(a, pltpu.HBM) for a in arrays]


def near(*arrays):
    return [pltpu.with_memory_space_constraint(a, pltpu.VMEM) for a in arrays]


def local(tracer_mass, send_ids, send_counts, sources, fractions, moments):
    count = lax.axis_size("curve")
    cells, width = tracer_mass.shape
    slots = send_ids.shape[1]
    elements = cells // 9
    plan = Plan(cells, width, elements, slots)
    lanes = plan.tiles * LANES
    src, fr, mo = sources.T, fractions.T, jnp.transpose(moments, (0, 2, 1))
    masses_t = pltpu.VMEM((cells, lanes), F32)
    weights_t = pltpu.VMEM((elements, LANES), F32)
    work_t = pltpu.VMEM((plan.tiles, cells, LANES), F32)
    payload, own_w, *pieces = pl.pallas_call(
        functools.partial(pack_kernel, plan),
        out_shape=(
            pltpu.VMEM((plan.rows, LANES), F32),
            weights_t,
            pltpu.VMEM(src.shape, jnp.int32),
            pltpu.VMEM(fr.shape, F32),
            pltpu.VMEM(mo.shape, F32),
        ),
        in_specs=[HBM] * 6,
        out_specs=(VMEM,) * 5,
        scratch_shapes=[
            pltpu.VMEM(tracer_mass.shape, F32),
            pltpu.VMEM(send_ids.shape, jnp.int32),
            pltpu.SMEM(send_counts.shape, jnp.int32),
            work_t,
            pltpu.SemaphoreType.DMA((6,)),
        ],
        compiler_params=GRANT,
        name="pack",
    )(*far(tracer_mass, src, fr, mo, send_ids, send_counts))

    def steps(by):
        pairs = [(i, i + (by if i % 2 else -by)) for i in range(count)]
        inside = [(i, j if 0 <= j < count else i ^ 1) for i, j in pairs]
        return inside, [(i, j % count) for i, j in pairs if not 0 <= j < count]

    towards, closing_x = steps(2)
    away, closing_y = steps(-2)
    swap = [(i, i ^ 1) for i in range(count)]
    closing = dict(closing_x + closing_y)
    closing = [(i, closing.get(i, i ^ 1)) for i in range(count)]
    index = lax.axis_index("curve")
    got_w = lax.ppermute(payload, "curve", closing)
    got_x = lax.ppermute(payload, "curve", towards)
    got_y = lax.ppermute(payload, "curve", away)
    shared = jnp.where((index == 1) | (index == count - 2), got_w, got_x)
    got_f = lax.ppermute(shared, "curve", swap)
    cost = pl.CostEstimate(flops=10**9, bytes_accessed=10**6, transcendentals=0)
    hi, lo = pl.pallas_call(
        functools.partial(matrix_kernel, plan),
        out_shape=(pltpu.VMEM((5, cells, cells), BF16),) * 2,
        in_specs=[VMEM] * 3,
        out_specs=(VMEM, VMEM),
        scratch_shapes=[pltpu.VMEM((cells, LANES), F32)],
        cost_estimate=cost,
        compiler_params=GRANT,
        name="matrix",
    )(*near(*pieces))
    acc, hot = pl.pallas_call(
        functools.partial(first_kernel, plan, count),
        out_shape=(masses_t, pltpu.VMEM((4, elements, slots), BF16)),
        in_specs=[VMEM, SMEM] + [VMEM] * 3,
        out_specs=(VMEM, VMEM),
        cost_estimate=cost,
        compiler_params=GRANT,
        name="first",
    )(send_ids, send_counts, *near(payload, hi, lo))
    weights = own_w
    for names, blocks in (("wx", (got_w, got_x)), ("f", (got_f,))):
        acc, weights = pl.pallas_call(
            functools.partial(next_kernel, plan, count, names),
            out_shape=(masses_t, weights_t),
            in_specs=[VMEM] * (5 + len(names)),
            out_specs=(VMEM, VMEM),
            cost_estimate=cost,
            compiler_params=GRANT,
        )(*near(acc, weights, hot, *blocks, hi, lo))
    return pl.pallas_call(
        functools.partial(last_kernel, plan, count, "y"),
        out_shape=jax.ShapeDtypeStruct((cells, width), F32),
        in_specs=[VMEM] * 7,
        out_specs=VMEM,
        scratch_shapes=[work_t],
        compiler_params=GRANT,
        name="last",
    )(*near(acc, weights, hot, payload, got_y, hi, lo))


def solution(mesh):
    placed = (
        P(("groups", "curve"), None),
        P(("groups", "curve"), None),
        P(("groups", "curve")),
        P(("groups", "curve"), None),
        P(("groups", "curve"), None),
        P(None, ("groups", "curve"), None),
    )
    return jax.shard_map(
        local, mesh=mesh, in_specs=placed, out_specs=P(("groups", "curve"), None), check_vma=False
    )
```

```python
import functools

import jax
import jax.numpy as jnp
from jax import lax
from jax.experimental import pallas as pl
from jax.experimental.pallas import tpu as pltpu
from jax.sharding import PartitionSpec as P


LANES = 128
F32 = jnp.float32
BF16 = jnp.bfloat16
GROUP = 28


def round8(n):
    return -(-n // 8) * 8


class Plan:
    def __init__(self, cells, width, elements, slots):
        self.cells, self.width, self.elements, self.slots = cells, width, elements, slots
        self.full = width // LANES
        rest = width % LANES
        self.rest = rest
        self.parts = []
        row = self.full * cells
        lane, size = 0, LANES // 2
        self.table = None
        while rest:
            if rest >= size:
                height = round8(-(-cells * size // LANES))
                if rest == size and height <= slots and -(-cells // slots) * size + 2 * GROUP <= LANES:
                    height, self.table, self.base = slots, row, -(-cells // slots) * size
                self.parts.append((lane, size, height, row))
                row += height
                lane += size
                rest -= size
            size //= 2
        if self.table is None:
            self.table, self.base = row, 0
            row += slots
        self.rows = row
        self.tiles = self.full + (1 if self.parts else 0)
        self.lanes = self.tiles * LANES

    def pack(self, tile_rows, outs):
        cells = self.cells
        lanes = lax.broadcasted_iota(jnp.int32, (1, LANES), 1)
        for t in range(self.full):
            tile = tile_rows(t)
            for out, _ in outs:
                out[t * cells:(t + 1) * cells, :] = tile
        if self.parts:
            last = tile_rows(self.full)
        for lane, size, height, first in self.parts:
            total = None
            for g in range(-(-cells // height)):
                count = min(height, cells - g * height)
                piece = last[g * height:g * height + count]
                shift = (g * size - lane) % LANES
                if shift:
                    piece = pltpu.roll(piece, shift, 1)
                if count < height:
                    piece = jnp.concatenate([piece, jnp.zeros((height - count, LANES), F32)], axis=0)
                total = piece if total is None else jnp.where(lanes >= g * size, piece, total)
            for out, table in outs:
                both = jnp.where(lanes >= self.base, table, total) if first == self.table else total
                out[first:first + height, :] = both
        if all(first != self.table for _, _, _, first in self.parts):
            for out, table in outs:
                out[self.table:self.rows, :] = table

    def unpack(self, ref):
        cells = self.cells
        tiles = [ref[t * cells:(t + 1) * cells, :] for t in range(self.full)]
        lanes = lax.broadcasted_iota(jnp.int32, (1, LANES), 1)
        if self.parts:
            last = None
            for lane, size, height, first in self.parts:
                block = ref[first:first + height, :]
                pieces = []
                for g in range(-(-cells // height)):
                    shift = (lane - g * size) % LANES
                    piece = pltpu.roll(block, shift, 1) if shift else block
                    pieces.append(piece[:min(height, cells - g * height)])
                piece = jnp.concatenate(pieces, axis=0)
                last = piece if last is None else jnp.where(lanes >= lane, piece, last)
            tiles.append(last)
        return jnp.concatenate(tiles, axis=1)


def split(x):
    high = x.astype(BF16)
    return high, (x - high.astype(F32)).astype(BF16)


def dot(a, b):
    return jnp.dot(a, b, preferred_element_type=F32)


def element_and_place(src):
    elem = ((src.astype(F32) + 0.5) * (1.0 / 9.0)).astype(jnp.int32)
    return elem, src - 9 * elem


def sent_list(name, count):
    index = lax.axis_index("curve")
    odd = lax.rem(index, 2) == 1
    end = (index == 0) | (index == count - 1)
    beside = (index == 1) | (index == count - 2)
    swap = jnp.where(odd, 2, 0)
    near = jnp.where(odd, 1, 3)
    far = jnp.where(odd, 3, 1)
    if name == "f":
        return jnp.where(odd, 0, 2)
    if name == "w":
        return jnp.where(end, near, jnp.where(beside, far, swap))
    if name == "x":
        return jnp.where(end, swap, near)
    return jnp.where(beside, swap, far)


def table_block(plan, tab_ref, name, count):
    at = plan.elements + plan.slots * lax.rem(sent_list(name, count) + 2, 4)
    return tab_ref[pl.ds(pl.multiple_of(at, 8), plan.slots), :]


def table_for(plan, tab_ref, name, count):
    lanes = lax.broadcasted_iota(jnp.int32, (1, LANES), 1)
    one = table_block(plan, tab_ref, name, count)
    one = pltpu.roll(one, plan.base, 1) if plan.base else one
    two = pltpu.roll(table_block(plan, tab_ref, "f", count), plan.base + GROUP, 1)
    return jnp.where(lanes >= plan.base + GROUP, two, one)


def pack_kernel(plan, count, q_hbm, src_hbm, fr_hbm, mo_hbm, ids_hbm, cnt_hbm,
                x_ref, w_ref, tab_ref, hot_ref, src_ref, fr_ref, mo_ref,
                q_ref, ids_ref, cnt_ref, t_ref, sems):
    E = plan.elements
    copies = [
        pltpu.make_async_copy(a, b, sems.at[n])
        for n, (a, b) in enumerate((
            (src_hbm, src_ref), (fr_hbm, fr_ref), (mo_hbm, mo_ref),
            (cnt_hbm, cnt_ref), (ids_hbm, ids_ref), (q_hbm, q_ref),
        ))
    ]
    for copy in copies:
        copy.start()
    for copy in copies[:5]:
        copy.wait()
    weights_table(plan, src_ref, fr_ref, mo_ref, ids_ref, cnt_ref, tab_ref)
    copies[5].wait()
    for t in range(plan.full):
        t_ref[t] = q_ref[:, t * LANES:(t + 1) * LANES]
    if plan.rest:
        t_ref[plan.full, :, 0:plan.rest] = q_ref[:, plan.full * LANES:plan.width]

    def tile_rows(t):
        return jnp.concatenate([t_ref[t, pl.ds(p, E, stride=9), :] for p in range(9)], axis=0)

    tables = [table_for(plan, tab_ref, name, count) for name in "xw"]
    plan.pack(tile_rows, ((x_ref, tables[0]), (w_ref, tables[1])))
    for n, name in enumerate("wxyf"):
        hot_ref[n] = live_slots(plan, my_list(name, count), ids_ref, cnt_ref)


def weights_table(plan, src_ref, fr_ref, mo_ref, ids_ref, cnt_ref, tab_ref):
    cells, E, S = plan.cells, plan.elements, plan.slots
    elem, place = element_and_place(src_ref[...])
    fr = fr_ref[...]
    wx = fr * mo_ref[0]
    wy = fr * mo_ref[1]
    total = E + 4 * S
    erow = lax.broadcasted_iota(jnp.int32, (total, cells), 0)
    urow = lax.broadcasted_iota(jnp.int32, (32, cells), 0)
    uplace = urow - jnp.where(urow < 9, 0, jnp.where(urow < 18, 9, 18))
    acc = None
    for k in range(src_ref.shape[0]):
        hot = jnp.where(erow == elem[k:k + 1, :], 1.0, 0.0).astype(BF16)
        value = jnp.where(urow < 9, fr[k:k + 1, :], jnp.where(urow < 18, wx[k:k + 1, :], wy[k:k + 1, :]))
        value = jnp.where(uplace == place[k:k + 1, :], value, 0.0)
        high, low = split(value)
        both = jnp.concatenate([high, low, jnp.zeros((64, cells), BF16)], axis=0)
        got = lax.dot_general(hot, both, (((1,), (1,)), ((), ())), preferred_element_type=F32)
        acc = got if acc is None else acc + got
    acc = acc + pltpu.roll(acc, LANES - 32, 1)
    tab_ref[0:E, :] = acc[0:E]
    lane = lax.broadcasted_iota(jnp.int32, (1, LANES), 1)
    diag = lax.broadcasted_iota(jnp.int32, (S, S), 0) == lax.broadcasted_iota(jnp.int32, (S, S), 1)
    slot = lax.broadcasted_iota(jnp.int32, (1, S), 1)
    for o in range(4):
        sent = (o + 2) % 4
        ids = jnp.where(slot < cnt_ref[sent], ids_ref[sent:sent + 1, :].astype(F32), -1.0)
        column = jnp.sum(jnp.where(diag, ids, 0.0), axis=1, keepdims=True)
        part = acc[E + o * S:E + (o + 1) * S]
        tab_ref[E + o * S:E + (o + 1) * S, :] = jnp.where(lane == GROUP - 1, column, part)


def matrix_kernel(plan, src_ref, fr_ref, mo_ref, mat_ref, col_ref):
    cells, E = plan.cells, plan.elements
    K = src_ref.shape[0]
    elem, place = element_and_place(src_ref[...])
    fr = fr_ref[...]
    wx = fr * mo_ref[0]
    wy = fr * mo_ref[1]
    row = jnp.where(place >= 6, 2, jnp.where(place >= 3, 1, 0))
    r = row.astype(F32)
    c = (place - 3 * row).astype(F32)
    centre = fr + wx * (c - 1.0) + wy * (r - 1.0)
    rows = [
        elem.astype(F32), place.astype(F32), centre,
        wx * (1.0 - 0.5 * c), wx * (-0.5 * c), wy * (1.0 - 0.5 * r), wy * (-0.5 * r),
    ]
    rows = jnp.concatenate(rows + [jnp.zeros((LANES - 7 * K, cells), F32)], axis=0)
    pad = -cells % LANES
    if pad:
        rows = jnp.concatenate([rows, jnp.zeros((LANES, pad), F32)], axis=1)
    col_ref[...] = jnp.transpose(rows, (1, 0))[0:cells]
    step = E
    lane = lax.broadcasted_iota(jnp.int32, (step, LANES), 1)
    per = LANES // E
    lists = mat_ref.shape[0]
    main = 8 * E

    def body(i, carry):
        at = pl.multiple_of(i * step, step)
        cols = col_ref[pl.ds(at, step), :]

        def wide(n, k):
            return jnp.broadcast_to(cols[:, n * K + k:n * K + k + 1], (step, LANES))

        inner = (lane % E).astype(F32)
        for t in range(main // LANES + 1):
            tail = t == main // LANES
            where = jnp.full((step, LANES), 8.0) if tail else (lane // E + per * t).astype(F32)
            sums = [jnp.zeros((step, LANES), F32) for _ in range(lists)]
            for k in range(K):
                d = where - wide(1, k)
                coef = jnp.where(d == 0.0, wide(2, k), 0.0)
                coef = jnp.where(d == 1.0, wide(3, k), coef)
                coef = jnp.where(d == 3.0, wide(5, k), coef)
                if not tail:
                    coef = jnp.where(d == -1.0, wide(4, k), coef)
                    coef = jnp.where(d == -3.0, wide(6, k), coef)
                e = wide(0, k) - inner
                for n in range(lists):
                    sums[n] = sums[n] + jnp.where(e == float(n * E), coef, 0.0)
            for n in range(lists):
                high, low = split(sums[n])
                if tail:
                    both = jnp.where(lane < 2 * E, high.astype(F32), low.astype(F32)).astype(BF16)
                    mat_ref[n, pl.ds(at, step), 2 * main:2 * main + LANES] = both
                else:
                    mat_ref[n, pl.ds(at, step), t * LANES:(t + 1) * LANES] = high
                    mat_ref[n, pl.ds(at, step), main + t * LANES:main + (t + 1) * LANES] = low
        return carry

    lax.fori_loop(0, cells // step, body, 0)


def in_slots(plan, masses, ids):
    E = plan.elements
    high, low = split(masses)
    per = LANES // E
    r = lax.broadcasted_iota(jnp.int32, (LANES, LANES), 0)
    l = lax.broadcasted_iota(jnp.int32, (LANES, LANES), 1)
    many = jnp.concatenate([ids] * per, axis=0)
    hot = jnp.where(((l % E).astype(F32) == many) & (r // E == l // E), 1.0, 0.0).astype(BF16)
    pair = jnp.concatenate([high, low], axis=1)
    pieces = []
    for first in range(0, plan.cells, LANES):
        size = min(LANES, plan.cells - first)
        pieces.append(dot(hot[:size, :size], pair[first:first + size]))
    pair = jnp.concatenate(pieces, axis=0)
    return pair[:, :plan.lanes], pair[:, plan.lanes:]


def product(plan, mat, high, low):
    E = plan.elements
    main = 8 * E
    ends = jnp.concatenate([high[main:], low[main:], high[main:]], axis=0)
    return (
        dot(mat[:, :main], high[:main]) + dot(mat[:, :main], low[:main])
        + dot(mat[:, main:2 * main], high[:main]) + dot(mat[:, 2 * main:2 * main + 3 * E], ends)
    )


def group_table(plan, block, group):
    at = plan.base + GROUP * group
    table = block[plan.table:plan.table + plan.slots, :]
    return pltpu.roll(table, LANES - at, 1) if at else table


def returned_weights(table, hot):
    lane = lax.broadcasted_iota(jnp.int32, table.shape, 1)
    high, low = split(jnp.where(lane < GROUP - 1, table, 0.0))
    return dot(hot, high) + dot(hot, low)


def live_slots(plan, which, ids_ref, cnt_ref):
    E, S = plan.elements, plan.slots
    slot = lax.broadcasted_iota(jnp.int32, (E, S), 1)
    e = lax.broadcasted_iota(jnp.int32, (E, S), 0)
    live = (e == ids_ref[pl.ds(which, 1), :]) & (slot < cnt_ref[which])
    return jnp.where(live, 1.0, 0.0).astype(BF16)


def my_list(name, count):
    index = lax.axis_index("curve")
    odd = lax.rem(index, 2) == 1
    end = (index == 0) | (index == count - 1)
    beside = (index == 1) | (index == count - 2)
    swap = jnp.where(odd, 2, 0)
    near = jnp.where(odd, 3, 1)
    far = jnp.where(odd, 1, 3)
    if name == "f":
        return jnp.where(odd, 0, 2)
    if name == "w":
        return jnp.where(end, far, jnp.where(beside, near, swap))
    if name == "x":
        return jnp.where(beside, swap, near)
    return jnp.where(end, swap, far)


def arrived(plan, name, count, block, hot_ref, mat_ref):
    theirs = lax.rem(my_list(name, count) + 2, 4)
    table = group_table(plan, block, 1 if name == "f" else 0)
    weights = returned_weights(table, hot_ref["wxyf".index(name)])
    masses = plan.unpack(block)
    if name == "y":
        high, low = split(masses)
    else:
        high, low = in_slots(plan, masses, table[:, GROUP - 1:GROUP])
        high, low = high.astype(BF16), low.astype(BF16)
    return product(plan, mat_ref[theirs + 1], high, low), weights


def kept(plan, masses, weights, out_ref):
    E = plan.elements
    for p in range(9):
        w = [jnp.broadcast_to(weights[:, 9 * j + p:9 * j + p + 1], (E, LANES)) for j in range(3)]
        for t in range(plan.tiles):
            def at(i):
                return masses[i * E:(i + 1) * E, t * LANES:(t + 1) * LANES]

            def slope(pos, step):
                if pos == 0:
                    return at(p + step) - at(p)
                if pos == 1:
                    return 0.5 * (at(p + step) - at(p - step))
                return at(p) - at(p - step)

            value = at(p) - (w[0] * at(p) + w[1] * slope(p % 3, 1) + w[2] * slope(p // 3, 3))
            out_ref[t, pl.ds(p, E, stride=9), :] = value


def listed_kernel(plan, count, tab_ref, own_ref, y_ref):
    ids = table_block(plan, tab_ref, "y", count)[:, GROUP - 1:GROUP]
    high, low = in_slots(plan, plan.unpack(own_ref), ids)
    listed = high + low
    plan.pack(lambda t: listed[:, t * LANES:(t + 1) * LANES], ((y_ref, table_for(plan, tab_ref, "y", count)),))


def own_kernel(plan, own_ref, mat_ref, acc_ref):
    acc_ref[...] = product(plan, mat_ref[0], *split(plan.unpack(own_ref)))


def pick_kernel(count, w_ref, x_ref, out_ref):
    index = lax.axis_index("curve")
    beside = (index == 1) | (index == count - 2)
    out_ref[...] = jnp.where(beside, w_ref[...], x_ref[...])


def next_kernel(plan, count, names, in_acc_ref, in_w_ref, hot_ref, mat_ref, *refs):
    blocks, (acc_ref, w_ref) = refs[:len(names)], refs[len(names):]
    acc, weights = in_acc_ref[...], in_w_ref[0:plan.elements, :]
    for name, ref in zip(names, blocks):
        more, extra = arrived(plan, name, count, ref, hot_ref, mat_ref)
        acc, weights = acc + more, weights + extra
    acc_ref[...] = acc
    w_ref[...] = weights


def last_kernel(plan, count, name, acc_ref, in_w_ref, hot_ref, mat_ref, own_ref, ref, out_ref, t_ref):
    more, weights = arrived(plan, name, count, ref, hot_ref, mat_ref)
    inflow = acc_ref[...] + more
    kept(plan, plan.unpack(own_ref), in_w_ref[...] + weights, t_ref)
    for t in range(plan.full):
        out_ref[:, t * LANES:(t + 1) * LANES] = t_ref[t] + inflow[:, t * LANES:(t + 1) * LANES]
    if plan.rest:
        at = plan.full * LANES
        out_ref[:, at:plan.width] = (t_ref[plan.full] + inflow[:, at:at + LANES])[:, :plan.rest]


GRANT = pltpu.CompilerParams(vmem_limit_bytes=8 * 2**20)
VMEM = pl.BlockSpec(memory_space=pltpu.VMEM)
SMEM = pl.BlockSpec(memory_space=pltpu.SMEM)


HBM = pl.BlockSpec(memory_space=pltpu.HBM)


def far(*arrays):
    return [pltpu.with_memory_space_constraint(a, pltpu.HBM) for a in arrays]


def near(*arrays):
    return [pltpu.with_memory_space_constraint(a, pltpu.VMEM) for a in arrays]


def local(tracer_mass, send_ids, send_counts, sources, fractions, moments):
    count = lax.axis_size("curve")
    cells, width = tracer_mass.shape
    slots = send_ids.shape[1]
    elements = cells // 9
    plan = Plan(cells, width, elements, slots)
    src, fr, mo = sources.T, fractions.T, jnp.transpose(moments, (0, 2, 1))
    payload_t = pltpu.VMEM((plan.rows, LANES), F32)
    masses_t = pltpu.VMEM((cells, plan.lanes), F32)
    weights_t = pltpu.VMEM((elements, LANES), F32)
    work_t = pltpu.VMEM((plan.tiles, cells, LANES), F32)
    pay_x, pay_w, table, hot, *pieces = pl.pallas_call(
        functools.partial(pack_kernel, plan, count),
        out_shape=(
            payload_t,
            payload_t,
            pltpu.VMEM((elements + 4 * slots, LANES), F32),
            pltpu.VMEM((4, elements, slots), BF16),
            pltpu.VMEM(src.shape, jnp.int32),
            pltpu.VMEM(fr.shape, F32),
            pltpu.VMEM(mo.shape, F32),
        ),
        in_specs=[HBM] * 6,
        out_specs=(VMEM,) * 7,
        scratch_shapes=[
            pltpu.VMEM(tracer_mass.shape, F32),
            pltpu.VMEM(send_ids.shape, jnp.int32),
            pltpu.SMEM(send_counts.shape, jnp.int32),
            work_t,
            pltpu.SemaphoreType.DMA((6,)),
        ],
        compiler_params=GRANT,
        name="pack",
    )(*far(tracer_mass, src, fr, mo, send_ids, send_counts))

    def steps(by):
        pairs = [(i, i + (by if i % 2 else -by)) for i in range(count)]
        inside = [(i, j if 0 <= j < count else i ^ 1) for i, j in pairs]
        return inside, [(i, j % count) for i, j in pairs if not 0 <= j < count]

    towards, closing_x = steps(2)
    away, closing_y = steps(-2)
    swap = [(i, i ^ 1) for i in range(count)]
    closing = dict(closing_x + closing_y)
    closing = [(i, closing.get(i, i ^ 1)) for i in range(count)]
    got_x = lax.ppermute(pay_x, "curve", towards)
    got_w = lax.ppermute(pay_w, "curve", closing)
    cost = pl.CostEstimate(flops=10**9, bytes_accessed=10**6, transcendentals=0)
    matrix = pl.pallas_call(
        functools.partial(matrix_kernel, plan),
        out_shape=pltpu.VMEM((5, cells, 16 * elements + LANES), BF16),
        in_specs=[VMEM] * 3,
        out_specs=VMEM,
        scratch_shapes=[pltpu.VMEM((cells, LANES), F32)],
        cost_estimate=cost,
        compiler_params=GRANT,
        name="matrix",
    )(*near(*pieces))
    pay_y = pl.pallas_call(
        functools.partial(listed_kernel, plan, count),
        out_shape=payload_t,
        in_specs=[VMEM] * 2,
        out_specs=VMEM,
        cost_estimate=cost,
        compiler_params=GRANT,
        name="listed",
    )(*near(table, pay_x))
    acc = pl.pallas_call(
        functools.partial(own_kernel, plan),
        out_shape=masses_t,
        in_specs=[VMEM] * 2,
        out_specs=VMEM,
        cost_estimate=cost,
        compiler_params=GRANT,
        name="own",
    )(*near(pay_x, matrix))
    got_y = lax.ppermute(pay_y, "curve", away)
    shared = pl.pallas_call(
        functools.partial(pick_kernel, count),
        out_shape=payload_t,
        in_specs=[VMEM] * 2,
        out_specs=VMEM,
        cost_estimate=cost,
        compiler_params=GRANT,
        name="pick",
    )(*near(got_w, got_x))
    got_f = lax.ppermute(shared, "curve", swap)
    weights = table
    for names, blocks in (("wx", (got_w, got_x)), ("f", (got_f,))):
        acc, weights = pl.pallas_call(
            functools.partial(next_kernel, plan, count, names),
            out_shape=(masses_t, weights_t),
            in_specs=[VMEM] * (4 + len(names)),
            out_specs=(VMEM, VMEM),
            input_output_aliases={0: 0},
            cost_estimate=cost,
            compiler_params=GRANT,
        )(*near(acc, weights, hot, matrix, *blocks))
    return pl.pallas_call(
        functools.partial(last_kernel, plan, count, "y"),
        out_shape=jax.ShapeDtypeStruct((cells, width), F32),
        in_specs=[VMEM] * 6,
        out_specs=VMEM,
        scratch_shapes=[work_t],
        compiler_params=GRANT,
        name="last",
    )(*near(acc, weights, hot, matrix, pay_x, got_y))


def solution(mesh):
    placed = (
        P(("groups", "curve"), None),
        P(("groups", "curve"), None),
        P(("groups", "curve")),
        P(("groups", "curve"), None),
        P(("groups", "curve"), None),
        P(None, ("groups", "curve"), None),
    )
    return jax.shard_map(
        local, mesh=mesh, in_specs=placed, out_specs=P(("groups", "curve"), None), check_vma=False
    )
```

```python
import functools

import jax
import jax.numpy as jnp
from jax import lax
from jax.experimental import pallas as pl
from jax.experimental.pallas import tpu as pltpu
from jax.sharding import PartitionSpec as P


LANES = 128
F32 = jnp.float32
BF16 = jnp.bfloat16
GROUP = 28


def round8(n):
    return -(-n // 8) * 8


class Plan:
    def __init__(self, cells, width, elements, slots):
        self.cells, self.width, self.elements, self.slots = cells, width, elements, slots
        self.full = width // LANES
        rest = width % LANES
        self.rest = rest
        self.parts = []
        row = self.full * cells
        lane, size = 0, LANES // 2
        self.table = None
        while rest:
            if rest >= size:
                height = round8(-(-cells * size // LANES))
                if rest == size and height <= slots and -(-cells // slots) * size + 2 * GROUP <= LANES:
                    height, self.table, self.base = slots, row, -(-cells // slots) * size
                self.parts.append((lane, size, height, row))
                row += height
                lane += size
                rest -= size
            size //= 2
        if self.table is None:
            self.table, self.base = row, 0
            row += slots
        self.rows = row
        self.tiles = self.full + (1 if self.parts else 0)
        self.lanes = self.tiles * LANES

    def pack(self, tile_rows, outs):
        cells = self.cells
        lanes = lax.broadcasted_iota(jnp.int32, (1, LANES), 1)
        for t in range(self.full):
            tile = tile_rows(t)
            for out, _ in outs:
                out[t * cells:(t + 1) * cells, :] = tile
        if self.parts:
            last = tile_rows(self.full)
        for lane, size, height, first in self.parts:
            total = None
            for g in range(-(-cells // height)):
                count = min(height, cells - g * height)
                piece = last[g * height:g * height + count]
                shift = (g * size - lane) % LANES
                if shift:
                    piece = pltpu.roll(piece, shift, 1)
                if count < height:
                    piece = jnp.concatenate([piece, jnp.zeros((height - count, LANES), F32)], axis=0)
                total = piece if total is None else jnp.where(lanes >= g * size, piece, total)
            for out, table in outs:
                both = jnp.where(lanes >= self.base, table, total) if first == self.table else total
                out[first:first + height, :] = both
        if all(first != self.table for _, _, _, first in self.parts):
            for out, table in outs:
                out[self.table:self.rows, :] = table

    def unpack(self, ref):
        cells = self.cells
        tiles = [ref[t * cells:(t + 1) * cells, :] for t in range(self.full)]
        lanes = lax.broadcasted_iota(jnp.int32, (1, LANES), 1)
        if self.parts:
            last = None
            for lane, size, height, first in self.parts:
                block = ref[first:first + height, :]
                pieces = []
                for g in range(-(-cells // height)):
                    shift = (lane - g * size) % LANES
                    piece = pltpu.roll(block, shift, 1) if shift else block
                    pieces.append(piece[:min(height, cells - g * height)])
                piece = jnp.concatenate(pieces, axis=0)
                last = piece if last is None else jnp.where(lanes >= lane, piece, last)
            tiles.append(last)
        return jnp.concatenate(tiles, axis=1)


def split(x):
    high = x.astype(BF16)
    return high, (x - high.astype(F32)).astype(BF16)


def dot(a, b):
    return jnp.dot(a, b, preferred_element_type=F32)


def element_and_place(src):
    elem = ((src.astype(F32) + 0.5) * (1.0 / 9.0)).astype(jnp.int32)
    return elem, src - 9 * elem


def sent_list(name, count):
    index = lax.axis_index("curve")
    odd = lax.rem(index, 2) == 1
    end = (index == 0) | (index == count - 1)
    beside = (index == 1) | (index == count - 2)
    swap = jnp.where(odd, 2, 0)
    near = jnp.where(odd, 1, 3)
    far = jnp.where(odd, 3, 1)
    if name == "f":
        return jnp.where(odd, 0, 2)
    if name == "w":
        return jnp.where(end, near, jnp.where(beside, far, swap))
    if name == "x":
        return jnp.where(end, swap, near)
    return jnp.where(beside, swap, far)


def table_block(plan, tab_ref, name, count):
    at = plan.elements + plan.slots * lax.rem(sent_list(name, count) + 2, 4)
    return tab_ref[pl.ds(pl.multiple_of(at, 8), plan.slots), :]


def table_for(plan, tab_ref, name, count):
    lanes = lax.broadcasted_iota(jnp.int32, (1, LANES), 1)
    one = table_block(plan, tab_ref, name, count)
    one = pltpu.roll(one, plan.base, 1) if plan.base else one
    two = pltpu.roll(table_block(plan, tab_ref, "f", count), plan.base + GROUP, 1)
    return jnp.where(lanes >= plan.base + GROUP, two, one)


def pack_kernel(plan, count, q_hbm, src_hbm, fr_hbm, mo_hbm, ids_hbm, cnt_hbm,
                x_ref, w_ref, tab_ref, hot_ref, src_ref, fr_ref, mo_ref,
                q_ref, ids_ref, cnt_ref, t_ref, sems):
    E = plan.elements
    copies = [
        pltpu.make_async_copy(a, b, sems.at[n])
        for n, (a, b) in enumerate((
            (src_hbm, src_ref), (fr_hbm, fr_ref), (mo_hbm, mo_ref),
            (cnt_hbm, cnt_ref), (ids_hbm, ids_ref), (q_hbm, q_ref),
        ))
    ]
    for copy in copies:
        copy.start()
    for copy in copies[:5]:
        copy.wait()
    weights_table(plan, src_ref, fr_ref, mo_ref, ids_ref, cnt_ref, tab_ref)
    copies[5].wait()
    for t in range(plan.full):
        t_ref[t] = q_ref[:, t * LANES:(t + 1) * LANES]
    if plan.rest:
        t_ref[plan.full, :, 0:plan.rest] = q_ref[:, plan.full * LANES:plan.width]

    def tile_rows(t):
        return jnp.concatenate([t_ref[t, pl.ds(p, E, stride=9), :] for p in range(9)], axis=0)

    tables = [table_for(plan, tab_ref, name, count) for name in "xw"]
    plan.pack(tile_rows, ((x_ref, tables[0]), (w_ref, tables[1])))
    for n, name in enumerate("wxyf"):
        hot_ref[n] = live_slots(plan, my_list(name, count), ids_ref, cnt_ref)


def weights_table(plan, src_ref, fr_ref, mo_ref, ids_ref, cnt_ref, tab_ref):
    cells, E, S = plan.cells, plan.elements, plan.slots
    elem, place = element_and_place(src_ref[...])
    fr = fr_ref[...]
    wx = fr * mo_ref[0]
    wy = fr * mo_ref[1]
    total = E + 4 * S
    erow = lax.broadcasted_iota(jnp.int32, (total, cells), 0)
    urow = lax.broadcasted_iota(jnp.int32, (32, cells), 0)
    uplace = urow - jnp.where(urow < 9, 0, jnp.where(urow < 18, 9, 18))
    acc = None
    for k in range(src_ref.shape[0]):
        hot = jnp.where(erow == elem[k:k + 1, :], 1.0, 0.0).astype(BF16)
        value = jnp.where(urow < 9, fr[k:k + 1, :], jnp.where(urow < 18, wx[k:k + 1, :], wy[k:k + 1, :]))
        value = jnp.where(uplace == place[k:k + 1, :], value, 0.0)
        high, low = split(value)
        both = jnp.concatenate([high, low, jnp.zeros((64, cells), BF16)], axis=0)
        got = lax.dot_general(hot, both, (((1,), (1,)), ((), ())), preferred_element_type=F32)
        acc = got if acc is None else acc + got
    acc = acc + pltpu.roll(acc, LANES - 32, 1)
    tab_ref[0:E, :] = acc[0:E]
    lane = lax.broadcasted_iota(jnp.int32, (1, LANES), 1)
    diag = lax.broadcasted_iota(jnp.int32, (S, S), 0) == lax.broadcasted_iota(jnp.int32, (S, S), 1)
    slot = lax.broadcasted_iota(jnp.int32, (1, S), 1)
    for o in range(4):
        sent = (o + 2) % 4
        ids = jnp.where(slot < cnt_ref[sent], ids_ref[sent:sent + 1, :].astype(F32), -1.0)
        column = jnp.sum(jnp.where(diag, ids, 0.0), axis=1, keepdims=True)
        part = acc[E + o * S:E + (o + 1) * S]
        tab_ref[E + o * S:E + (o + 1) * S, :] = jnp.where(lane == GROUP - 1, column, part)


def matrix_kernel(plan, src_ref, fr_ref, mo_ref, mat_ref, col_ref):
    cells, E = plan.cells, plan.elements
    K = src_ref.shape[0]
    elem, place = element_and_place(src_ref[...])
    fr = fr_ref[...]
    wx = fr * mo_ref[0]
    wy = fr * mo_ref[1]
    row = jnp.where(place >= 6, 2, jnp.where(place >= 3, 1, 0))
    r = row.astype(F32)
    c = (place - 3 * row).astype(F32)
    centre = fr + wx * (c - 1.0) + wy * (r - 1.0)
    rows = [
        elem.astype(F32), place.astype(F32), centre,
        wx * (1.0 - 0.5 * c), wx * (-0.5 * c), wy * (1.0 - 0.5 * r), wy * (-0.5 * r),
    ]
    rows = jnp.concatenate(rows + [jnp.zeros((LANES - 7 * K, cells), F32)], axis=0)
    pad = -cells % LANES
    if pad:
        rows = jnp.concatenate([rows, jnp.zeros((LANES, pad), F32)], axis=1)
    col_ref[...] = jnp.transpose(rows, (1, 0))[0:cells]
    step = E
    lane = lax.broadcasted_iota(jnp.int32, (step, LANES), 1)
    per = LANES // E
    lists = mat_ref.shape[0]
    main = 8 * E

    def body(i, carry):
        at = pl.multiple_of(i * step, step)
        cols = col_ref[pl.ds(at, step), :]

        def wide(n, k):
            return jnp.broadcast_to(cols[:, n * K + k:n * K + k + 1], (step, LANES))

        inner = (lane % E).astype(F32)
        for t in range(main // LANES + 1):
            tail = t == main // LANES
            where = jnp.full((step, LANES), 8.0) if tail else (lane // E + per * t).astype(F32)
            sums = [jnp.zeros((step, LANES), F32) for _ in range(lists)]
            for k in range(K):
                d = where - wide(1, k)
                coef = jnp.where(d == 0.0, wide(2, k), 0.0)
                coef = jnp.where(d == 1.0, wide(3, k), coef)
                coef = jnp.where(d == 3.0, wide(5, k), coef)
                if not tail:
                    coef = jnp.where(d == -1.0, wide(4, k), coef)
                    coef = jnp.where(d == -3.0, wide(6, k), coef)
                e = wide(0, k) - inner
                for n in range(lists):
                    sums[n] = sums[n] + jnp.where(e == float(n * E), coef, 0.0)
            for n in range(lists):
                high, low = split(sums[n])
                if tail:
                    both = jnp.where(lane < 2 * E, high.astype(F32), low.astype(F32)).astype(BF16)
                    mat_ref[n, pl.ds(at, step), 2 * main:2 * main + LANES] = both
                else:
                    mat_ref[n, pl.ds(at, step), t * LANES:(t + 1) * LANES] = high
                    mat_ref[n, pl.ds(at, step), main + t * LANES:main + (t + 1) * LANES] = low
        return carry

    lax.fori_loop(0, cells // step, body, 0)


def in_slots(plan, masses, ids):
    E = plan.elements
    high, low = split(masses)
    per = LANES // E
    r = lax.broadcasted_iota(jnp.int32, (LANES, LANES), 0)
    l = lax.broadcasted_iota(jnp.int32, (LANES, LANES), 1)
    many = jnp.concatenate([ids] * per, axis=0)
    hot = jnp.where(((l % E).astype(F32) == many) & (r // E == l // E), 1.0, 0.0).astype(BF16)
    pair = jnp.concatenate([high, low], axis=1)
    pieces = []
    for first in range(0, plan.cells, LANES):
        size = min(LANES, plan.cells - first)
        pieces.append(dot(hot[:size, :size], pair[first:first + size]))
    pair = jnp.concatenate(pieces, axis=0)
    return pair[:, :plan.lanes], pair[:, plan.lanes:]


def product(plan, mat, high, low):
    E = plan.elements
    main = 8 * E
    ends = jnp.concatenate([high[main:], low[main:], high[main:]], axis=0)
    return (
        dot(mat[:, :main], high[:main]) + dot(mat[:, :main], low[:main])
        + dot(mat[:, main:2 * main], high[:main]) + dot(mat[:, 2 * main:2 * main + 3 * E], ends)
    )


def group_table(plan, block, group):
    at = plan.base + GROUP * group
    table = block[plan.table:plan.table + plan.slots, :]
    return pltpu.roll(table, LANES - at, 1) if at else table


def returned_weights(table, hot):
    lane = lax.broadcasted_iota(jnp.int32, table.shape, 1)
    high, low = split(jnp.where(lane < GROUP - 1, table, 0.0))
    return dot(hot, high) + dot(hot, low)


def live_slots(plan, which, ids_ref, cnt_ref):
    E, S = plan.elements, plan.slots
    slot = lax.broadcasted_iota(jnp.int32, (E, S), 1)
    e = lax.broadcasted_iota(jnp.int32, (E, S), 0)
    live = (e == ids_ref[pl.ds(which, 1), :]) & (slot < cnt_ref[which])
    return jnp.where(live, 1.0, 0.0).astype(BF16)


def my_list(name, count):
    index = lax.axis_index("curve")
    odd = lax.rem(index, 2) == 1
    end = (index == 0) | (index == count - 1)
    beside = (index == 1) | (index == count - 2)
    swap = jnp.where(odd, 2, 0)
    near = jnp.where(odd, 3, 1)
    far = jnp.where(odd, 1, 3)
    if name == "f":
        return jnp.where(odd, 0, 2)
    if name == "w":
        return jnp.where(end, far, jnp.where(beside, near, swap))
    if name == "x":
        return jnp.where(beside, swap, near)
    return jnp.where(end, swap, far)


def arrived(plan, name, count, block, hot_ref, mat_ref):
    theirs = lax.rem(my_list(name, count) + 2, 4)
    table = group_table(plan, block, 1 if name == "f" else 0)
    weights = returned_weights(table, hot_ref["wxyf".index(name)])
    masses = plan.unpack(block)
    if name in "fy":
        high, low = split(masses)
    else:
        high, low = in_slots(plan, masses, table[:, GROUP - 1:GROUP])
        high, low = high.astype(BF16), low.astype(BF16)
    return product(plan, mat_ref[theirs + 1], high, low), weights


def kept(plan, masses, weights, out_ref):
    E = plan.elements
    for p in range(9):
        w = [jnp.broadcast_to(weights[:, 9 * j + p:9 * j + p + 1], (E, LANES)) for j in range(3)]
        for t in range(plan.tiles):
            def at(i):
                return masses[i * E:(i + 1) * E, t * LANES:(t + 1) * LANES]

            def slope(pos, step):
                if pos == 0:
                    return at(p + step) - at(p)
                if pos == 1:
                    return 0.5 * (at(p + step) - at(p - step))
                return at(p) - at(p - step)

            value = at(p) - (w[0] * at(p) + w[1] * slope(p % 3, 1) + w[2] * slope(p // 3, 3))
            out_ref[t, pl.ds(p, E, stride=9), :] = value


def listed_kernel(plan, count, tab_ref, own_ref, y_ref):
    ids = table_block(plan, tab_ref, "y", count)[:, GROUP - 1:GROUP]
    high, low = in_slots(plan, plan.unpack(own_ref), ids)
    listed = high + low
    plan.pack(lambda t: listed[:, t * LANES:(t + 1) * LANES], ((y_ref, table_for(plan, tab_ref, "y", count)),))


def own_kernel(plan, own_ref, mat_ref, acc_ref):
    acc_ref[...] = product(plan, mat_ref[0], *split(plan.unpack(own_ref)))


def reorder(plan, ref, out_ref):
    ids = group_table(plan, ref, 1)[:, GROUP - 1:GROUP]
    high, low = in_slots(plan, plan.unpack(ref), ids)
    listed = high + low
    table = ref[plan.table:plan.table + plan.slots, :]
    plan.pack(lambda t: listed[:, t * LANES:(t + 1) * LANES], ((out_ref, table),))


def shared_kernel(plan, x_ref, out_ref):
    reorder(plan, x_ref, out_ref)


def pick_kernel(plan, count, w_ref, x_ref, out_ref):
    index = lax.axis_index("curve")
    beside = (index == 1) | (index == count - 2)
    pl.when(beside)(lambda: reorder(plan, w_ref, out_ref))

    @pl.when(jnp.logical_not(beside))
    def _():
        out_ref[...] = x_ref[...]


def all_at_once():
    return lax.axis_index("curve") == 0


def next_kernel(plan, count, name, in_acc_ref, in_w_ref, hot_ref, mat_ref, ref, acc_ref, w_ref):
    def work_off():
        acc, weights = in_acc_ref[...], in_w_ref[0:plan.elements, :]
        more, extra = arrived(plan, name, count, ref, hot_ref, mat_ref)
        acc_ref[...] = acc + more
        w_ref[...] = weights + extra

    if name != "f":
        return work_off()
    pl.when(jnp.logical_not(all_at_once()))(work_off)

    @pl.when(all_at_once())
    def _():
        acc_ref[...] = in_acc_ref[...]
        w_ref[...] = in_w_ref[...]


def last_kernel(plan, count, acc_ref, in_w_ref, hot_ref, mat_ref, own_ref, f_ref, y_ref, out_ref, t_ref):
    def work_off(names):
        inflow, weights = acc_ref[...], in_w_ref[...]
        for name in names:
            more, extra = arrived(plan, name, count, f_ref if name == "f" else y_ref, hot_ref, mat_ref)
            inflow, weights = inflow + more, weights + extra
        kept(plan, plan.unpack(own_ref), weights, t_ref)
        for t in range(plan.full):
            out_ref[:, t * LANES:(t + 1) * LANES] = t_ref[t] + inflow[:, t * LANES:(t + 1) * LANES]
        if plan.rest:
            at = plan.full * LANES
            out_ref[:, at:plan.width] = (t_ref[plan.full] + inflow[:, at:at + LANES])[:, :plan.rest]

    pl.when(all_at_once())(lambda: work_off("fy"))
    pl.when(jnp.logical_not(all_at_once()))(lambda: work_off("y"))


GRANT = pltpu.CompilerParams(vmem_limit_bytes=8 * 2**20)
VMEM = pl.BlockSpec(memory_space=pltpu.VMEM)
SMEM = pl.BlockSpec(memory_space=pltpu.SMEM)


HBM = pl.BlockSpec(memory_space=pltpu.HBM)


def far(*arrays):
    return [pltpu.with_memory_space_constraint(a, pltpu.HBM) for a in arrays]


def near(*arrays):
    return [pltpu.with_memory_space_constraint(a, pltpu.VMEM) for a in arrays]


def local(tracer_mass, send_ids, send_counts, sources, fractions, moments):
    count = lax.axis_size("curve")
    cells, width = tracer_mass.shape
    slots = send_ids.shape[1]
    elements = cells // 9
    plan = Plan(cells, width, elements, slots)
    src, fr, mo = sources.T, fractions.T, jnp.transpose(moments, (0, 2, 1))
    payload_t = pltpu.VMEM((plan.rows, LANES), F32)
    masses_t = pltpu.VMEM((cells, plan.lanes), F32)
    weights_t = pltpu.VMEM((elements, LANES), F32)
    work_t = pltpu.VMEM((plan.tiles, cells, LANES), F32)
    pay_x, pay_w, table, hot, *pieces = pl.pallas_call(
        functools.partial(pack_kernel, plan, count),
        out_shape=(
            payload_t,
            payload_t,
            pltpu.VMEM((elements + 4 * slots, LANES), F32),
            pltpu.VMEM((4, elements, slots), BF16),
            pltpu.VMEM(src.shape, jnp.int32),
            pltpu.VMEM(fr.shape, F32),
            pltpu.VMEM(mo.shape, F32),
        ),
        in_specs=[HBM] * 6,
        out_specs=(VMEM,) * 7,
        scratch_shapes=[
            pltpu.VMEM(tracer_mass.shape, F32),
            pltpu.VMEM(send_ids.shape, jnp.int32),
            pltpu.SMEM(send_counts.shape, jnp.int32),
            work_t,
            pltpu.SemaphoreType.DMA((6,)),
        ],
        compiler_params=GRANT,
        name="pack",
    )(*far(tracer_mass, src, fr, mo, send_ids, send_counts))

    def steps(by):
        pairs = [(i, i + (by if i % 2 else -by)) for i in range(count)]
        inside = [(i, j if 0 <= j < count else i ^ 1) for i, j in pairs]
        return inside, [(i, j % count) for i, j in pairs if not 0 <= j < count]

    towards, closing_x = steps(2)
    away, closing_y = steps(-2)
    swap = [(i, i ^ 1) for i in range(count)]
    closing = dict(closing_x + closing_y)
    closing = [(i, closing.get(i, i ^ 1)) for i in range(count)]
    got_x = lax.ppermute(pay_x, "curve", towards)
    got_w = lax.ppermute(pay_w, "curve", closing)
    cost = pl.CostEstimate(flops=10**9, bytes_accessed=10**6, transcendentals=0)
    matrix = pl.pallas_call(
        functools.partial(matrix_kernel, plan),
        out_shape=pltpu.VMEM((5, cells, 16 * elements + LANES), BF16),
        in_specs=[VMEM] * 3,
        out_specs=VMEM,
        scratch_shapes=[pltpu.VMEM((cells, LANES), F32)],
        cost_estimate=cost,
        compiler_params=GRANT,
        name="matrix",
    )(*near(*pieces))
    pay_y = pl.pallas_call(
        functools.partial(listed_kernel, plan, count),
        out_shape=payload_t,
        in_specs=[VMEM] * 2,
        out_specs=VMEM,
        cost_estimate=cost,
        compiler_params=GRANT,
        name="listed",
    )(*near(table, pay_x))
    acc = pl.pallas_call(
        functools.partial(own_kernel, plan),
        out_shape=masses_t,
        in_specs=[VMEM] * 2,
        out_specs=VMEM,
        cost_estimate=cost,
        compiler_params=GRANT,
        name="own",
    )(*near(pay_x, matrix))
    got_y = lax.ppermute(pay_y, "curve", away)
    shared = pl.pallas_call(
        functools.partial(shared_kernel, plan),
        out_shape=payload_t,
        in_specs=[VMEM],
        out_specs=VMEM,
        cost_estimate=cost,
        compiler_params=GRANT,
        name="shared",
    )(*near(got_x))
    shared = pl.pallas_call(
        functools.partial(pick_kernel, plan, count),
        out_shape=payload_t,
        in_specs=[VMEM] * 2,
        out_specs=VMEM,
        cost_estimate=cost,
        compiler_params=GRANT,
        name="pick",
    )(*near(got_w, shared))
    got_f = lax.ppermute(shared, "curve", swap)
    weights = table
    for name, block in (("x", got_x), ("w", got_w), ("f", got_f)):
        acc, weights = pl.pallas_call(
            functools.partial(next_kernel, plan, count, name),
            out_shape=(masses_t, weights_t),
            in_specs=[VMEM] * 5,
            out_specs=(VMEM, VMEM),
            input_output_aliases={0: 0},
            cost_estimate=cost,
            compiler_params=GRANT,
        )(*near(acc, weights, hot, matrix, block))
    return pl.pallas_call(
        functools.partial(last_kernel, plan, count),
        out_shape=jax.ShapeDtypeStruct((cells, width), F32),
        in_specs=[VMEM] * 7,
        out_specs=VMEM,
        scratch_shapes=[work_t],
        compiler_params=GRANT,
        name="last",
    )(*near(acc, weights, hot, matrix, pay_x, got_f, got_y))


def solution(mesh):
    placed = (
        P(("groups", "curve"), None),
        P(("groups", "curve"), None),
        P(("groups", "curve")),
        P(("groups", "curve"), None),
        P(("groups", "curve"), None),
        P(None, ("groups", "curve"), None),
    )
    return jax.shard_map(
        local, mesh=mesh, in_specs=placed, out_specs=P(("groups", "curve"), None), check_vma=False
    )
```

```python
import functools

import jax
import jax.numpy as jnp
from jax import lax
from jax.experimental import pallas as pl
from jax.experimental.pallas import tpu as pltpu
from jax.sharding import PartitionSpec as P


LANES = 128
F32 = jnp.float32
BF16 = jnp.bfloat16
GROUP = 28


def round8(n):
    return -(-n // 8) * 8


class Plan:
    def __init__(self, cells, width, elements, slots):
        self.cells, self.width, self.elements, self.slots = cells, width, elements, slots
        self.full = width // LANES
        rest = width % LANES
        self.rest = rest
        self.parts = []
        row = self.full * cells
        lane, size = 0, LANES // 2
        self.table = None
        while rest:
            if rest >= size:
                height = round8(-(-cells * size // LANES))
                if rest == size and height <= slots and -(-cells // slots) * size + 2 * GROUP <= LANES:
                    height, self.table, self.base = slots, row, -(-cells // slots) * size
                self.parts.append((lane, size, height, row))
                row += height
                lane += size
                rest -= size
            size //= 2
        if self.table is None:
            self.table, self.base = row, 0
            row += slots
        self.rows = row
        self.tiles = self.full + (1 if self.parts else 0)
        self.lanes = self.tiles * LANES

    def pack(self, tile_rows, outs):
        cells = self.cells
        lanes = lax.broadcasted_iota(jnp.int32, (1, LANES), 1)
        for t in range(self.full):
            tile = tile_rows(t)
            for out, _ in outs:
                out[t * cells:(t + 1) * cells, :] = tile
        if self.parts:
            last = tile_rows(self.full)
        for lane, size, height, first in self.parts:
            total = None
            for g in range(-(-cells // height)):
                count = min(height, cells - g * height)
                piece = last[g * height:g * height + count]
                shift = (g * size - lane) % LANES
                if shift:
                    piece = pltpu.roll(piece, shift, 1)
                if count < height:
                    piece = jnp.concatenate([piece, jnp.zeros((height - count, LANES), F32)], axis=0)
                total = piece if total is None else jnp.where(lanes >= g * size, piece, total)
            for out, table in outs:
                both = jnp.where(lanes >= self.base, table, total) if first == self.table else total
                out[first:first + height, :] = both
        if all(first != self.table for _, _, _, first in self.parts):
            for out, table in outs:
                out[self.table:self.rows, :] = table

    def unpack(self, ref):
        cells = self.cells
        tiles = [ref[t * cells:(t + 1) * cells, :] for t in range(self.full)]
        lanes = lax.broadcasted_iota(jnp.int32, (1, LANES), 1)
        if self.parts:
            last = None
            for lane, size, height, first in self.parts:
                block = ref[first:first + height, :]
                pieces = []
                for g in range(-(-cells // height)):
                    shift = (lane - g * size) % LANES
                    piece = pltpu.roll(block, shift, 1) if shift else block
                    pieces.append(piece[:min(height, cells - g * height)])
                piece = jnp.concatenate(pieces, axis=0)
                last = piece if last is None else jnp.where(lanes >= lane, piece, last)
            tiles.append(last)
        return jnp.concatenate(tiles, axis=1)


def split(x):
    high = x.astype(BF16)
    return high, (x - high.astype(F32)).astype(BF16)


def dot(a, b):
    return jnp.dot(a, b, preferred_element_type=F32)


def element_and_place(src):
    elem = ((src.astype(F32) + 0.5) * (1.0 / 9.0)).astype(jnp.int32)
    return elem, src - 9 * elem


def sent_list(name, count):
    index = lax.axis_index("curve")
    odd = lax.rem(index, 2) == 1
    end = (index == 0) | (index == count - 1)
    beside = (index == 1) | (index == count - 2)
    swap = jnp.where(odd, 2, 0)
    near = jnp.where(odd, 1, 3)
    far = jnp.where(odd, 3, 1)
    if name == "f":
        return jnp.where(odd, 0, 2)
    if name == "w":
        return jnp.where(end, near, jnp.where(beside, far, swap))
    if name == "x":
        return jnp.where(end, swap, near)
    return jnp.where(beside, swap, far)


def table_block(plan, tab_ref, name, count):
    at = plan.elements + plan.slots * lax.rem(sent_list(name, count) + 2, 4)
    return tab_ref[pl.ds(pl.multiple_of(at, 8), plan.slots), :]


def table_for(plan, tab_ref, name, count):
    lanes = lax.broadcasted_iota(jnp.int32, (1, LANES), 1)
    one = table_block(plan, tab_ref, name, count)
    one = pltpu.roll(one, plan.base, 1) if plan.base else one
    two = pltpu.roll(table_block(plan, tab_ref, "f", count), plan.base + GROUP, 1)
    return jnp.where(lanes >= plan.base + GROUP, two, one)


def pack_kernel(plan, count, q_hbm, src_hbm, fr_hbm, mo_hbm, ids_hbm, cnt_hbm,
                x_ref, w_ref, tab_ref, hot_ref, src_ref, fr_ref, mo_ref,
                q_ref, ids_ref, cnt_ref, t_ref, sems):
    E = plan.elements
    copies = [
        pltpu.make_async_copy(a, b, sems.at[n])
        for n, (a, b) in enumerate((
            (src_hbm, src_ref), (fr_hbm, fr_ref), (mo_hbm, mo_ref),
            (cnt_hbm, cnt_ref), (ids_hbm, ids_ref), (q_hbm, q_ref),
        ))
    ]
    for copy in copies:
        copy.start()
    for copy in copies[:5]:
        copy.wait()
    weights_table(plan, src_ref, fr_ref, mo_ref, ids_ref, cnt_ref, tab_ref)
    copies[5].wait()
    for t in range(plan.full):
        t_ref[t] = q_ref[:, t * LANES:(t + 1) * LANES]
    if plan.rest:
        t_ref[plan.full, :, 0:plan.rest] = q_ref[:, plan.full * LANES:plan.width]

    def tile_rows(t):
        return jnp.concatenate([t_ref[t, pl.ds(p, E, stride=9), :] for p in range(9)], axis=0)

    tables = [table_for(plan, tab_ref, name, count) for name in "xw"]
    plan.pack(tile_rows, ((x_ref, tables[0]), (w_ref, tables[1])))
    for n, name in enumerate("wxyf"):
        hot_ref[n] = live_slots(plan, my_list(name, count), ids_ref, cnt_ref)


def weights_table(plan, src_ref, fr_ref, mo_ref, ids_ref, cnt_ref, tab_ref):
    cells, E, S = plan.cells, plan.elements, plan.slots
    elem, place = element_and_place(src_ref[...])
    fr = fr_ref[...]
    wx = fr * mo_ref[0]
    wy = fr * mo_ref[1]
    total = E + 4 * S
    erow = lax.broadcasted_iota(jnp.int32, (total, cells), 0)
    urow = lax.broadcasted_iota(jnp.int32, (32, cells), 0)
    uplace = urow - jnp.where(urow < 9, 0, jnp.where(urow < 18, 9, 18))
    acc = None
    for k in range(src_ref.shape[0]):
        hot = jnp.where(erow == elem[k:k + 1, :], 1.0, 0.0).astype(BF16)
        value = jnp.where(urow < 9, fr[k:k + 1, :], jnp.where(urow < 18, wx[k:k + 1, :], wy[k:k + 1, :]))
        value = jnp.where(uplace == place[k:k + 1, :], value, 0.0)
        high, low = split(value)
        both = jnp.concatenate([high, low, jnp.zeros((64, cells), BF16)], axis=0)
        got = lax.dot_general(hot, both, (((1,), (1,)), ((), ())), preferred_element_type=F32)
        acc = got if acc is None else acc + got
    acc = acc + pltpu.roll(acc, LANES - 32, 1)
    tab_ref[0:E, :] = acc[0:E]
    lane = lax.broadcasted_iota(jnp.int32, (1, LANES), 1)
    diag = lax.broadcasted_iota(jnp.int32, (S, S), 0) == lax.broadcasted_iota(jnp.int32, (S, S), 1)
    slot = lax.broadcasted_iota(jnp.int32, (1, S), 1)
    for o in range(4):
        sent = (o + 2) % 4
        ids = jnp.where(slot < cnt_ref[sent], ids_ref[sent:sent + 1, :].astype(F32), -1.0)
        column = jnp.sum(jnp.where(diag, ids, 0.0), axis=1, keepdims=True)
        part = acc[E + o * S:E + (o + 1) * S]
        tab_ref[E + o * S:E + (o + 1) * S, :] = jnp.where(lane == GROUP - 1, column, part)


def matrix_kernel(plan, src_ref, fr_ref, mo_ref, mat_ref, col_ref):
    cells, E = plan.cells, plan.elements
    K = src_ref.shape[0]
    elem, place = element_and_place(src_ref[...])
    fr = fr_ref[...]
    wx = fr * mo_ref[0]
    wy = fr * mo_ref[1]
    row = jnp.where(place >= 6, 2, jnp.where(place >= 3, 1, 0))
    r = row.astype(F32)
    c = (place - 3 * row).astype(F32)
    centre = fr + wx * (c - 1.0) + wy * (r - 1.0)
    rows = [
        elem.astype(F32), place.astype(F32), centre,
        wx * (1.0 - 0.5 * c), wx * (-0.5 * c), wy * (1.0 - 0.5 * r), wy * (-0.5 * r),
    ]
    rows = jnp.concatenate(rows + [jnp.zeros((LANES - 7 * K, cells), F32)], axis=0)
    pad = -cells % LANES
    if pad:
        rows = jnp.concatenate([rows, jnp.zeros((LANES, pad), F32)], axis=1)
    col_ref[...] = jnp.transpose(rows, (1, 0))[0:cells]
    step = E
    lane = lax.broadcasted_iota(jnp.int32, (step, LANES), 1)
    per = LANES // E
    lists = mat_ref.shape[0]
    main = 8 * E

    def body(i, carry):
        at = pl.multiple_of(i * step, step)
        cols = col_ref[pl.ds(at, step), :]

        def wide(n, k):
            return jnp.broadcast_to(cols[:, n * K + k:n * K + k + 1], (step, LANES))

        inner = (lane % E).astype(F32)
        for t in range(main // LANES + 1):
            tail = t == main // LANES
            where = jnp.full((step, LANES), 8.0) if tail else (lane // E + per * t).astype(F32)
            sums = [jnp.zeros((step, LANES), F32) for _ in range(lists)]
            for k in range(K):
                d = where - wide(1, k)
                coef = jnp.where(d == 0.0, wide(2, k), 0.0)
                coef = jnp.where(d == 1.0, wide(3, k), coef)
                coef = jnp.where(d == 3.0, wide(5, k), coef)
                if not tail:
                    coef = jnp.where(d == -1.0, wide(4, k), coef)
                    coef = jnp.where(d == -3.0, wide(6, k), coef)
                e = wide(0, k) - inner
                for n in range(lists):
                    sums[n] = sums[n] + jnp.where(e == float(n * E), coef, 0.0)
            for n in range(lists):
                high, low = split(sums[n])
                if tail:
                    both = jnp.where(lane < 2 * E, high.astype(F32), low.astype(F32)).astype(BF16)
                    mat_ref[n, pl.ds(at, step), 2 * main:2 * main + LANES] = both
                else:
                    mat_ref[n, pl.ds(at, step), t * LANES:(t + 1) * LANES] = high
                    mat_ref[n, pl.ds(at, step), main + t * LANES:main + (t + 1) * LANES] = low
        return carry

    lax.fori_loop(0, cells // step, body, 0)


def in_slots(plan, masses, ids):
    E = plan.elements
    high, low = split(masses)
    per = LANES // E
    r = lax.broadcasted_iota(jnp.int32, (LANES, LANES), 0)
    l = lax.broadcasted_iota(jnp.int32, (LANES, LANES), 1)
    many = jnp.concatenate([ids] * per, axis=0)
    hot = jnp.where(((l % E).astype(F32) == many) & (r // E == l // E), 1.0, 0.0).astype(BF16)
    pair = jnp.concatenate([high, low], axis=1)
    pieces = []
    for first in range(0, plan.cells, LANES):
        size = min(LANES, plan.cells - first)
        pieces.append(dot(hot[:size, :size], pair[first:first + size]))
    pair = jnp.concatenate(pieces, axis=0)
    return pair[:, :plan.lanes], pair[:, plan.lanes:]


def product(plan, mat, high, low):
    E = plan.elements
    main = 8 * E
    ends = jnp.concatenate([high[main:], low[main:], high[main:]], axis=0)
    return (
        dot(mat[:, :main], high[:main]) + dot(mat[:, :main], low[:main])
        + dot(mat[:, main:2 * main], high[:main]) + dot(mat[:, 2 * main:2 * main + 3 * E], ends)
    )


def group_table(plan, block, group):
    at = plan.base + GROUP * group
    table = block[plan.table:plan.table + plan.slots, :]
    return pltpu.roll(table, LANES - at, 1) if at else table


def returned_weights(table, hot):
    lane = lax.broadcasted_iota(jnp.int32, table.shape, 1)
    high, low = split(jnp.where(lane < GROUP - 1, table, 0.0))
    return dot(hot, high) + dot(hot, low)


def live_slots(plan, which, ids_ref, cnt_ref):
    E, S = plan.elements, plan.slots
    slot = lax.broadcasted_iota(jnp.int32, (E, S), 1)
    e = lax.broadcasted_iota(jnp.int32, (E, S), 0)
    live = (e == ids_ref[pl.ds(which, 1), :]) & (slot < cnt_ref[which])
    return jnp.where(live, 1.0, 0.0).astype(BF16)


def my_list(name, count):
    index = lax.axis_index("curve")
    odd = lax.rem(index, 2) == 1
    end = (index == 0) | (index == count - 1)
    beside = (index == 1) | (index == count - 2)
    swap = jnp.where(odd, 2, 0)
    near = jnp.where(odd, 3, 1)
    far = jnp.where(odd, 1, 3)
    if name == "f":
        return jnp.where(odd, 0, 2)
    if name == "w":
        return jnp.where(end, far, jnp.where(beside, near, swap))
    if name == "x":
        return jnp.where(beside, swap, near)
    return jnp.where(end, swap, far)


def arrived(plan, name, count, block, hot_ref, mat_ref):
    theirs = lax.rem(my_list(name, count) + 2, 4)
    table = group_table(plan, block, 1 if name == "f" else 0)
    weights = returned_weights(table, hot_ref["wxyf".index(name)])
    masses = plan.unpack(block)
    if name in "fy":
        high, low = split(masses)
    else:
        high, low = in_slots(plan, masses, table[:, GROUP - 1:GROUP])
        high, low = high.astype(BF16), low.astype(BF16)
    return product(plan, mat_ref[theirs + 1], high, low), weights


def kept(plan, masses, weights, out_ref):
    E = plan.elements
    for p in range(9):
        w = [jnp.broadcast_to(weights[:, 9 * j + p:9 * j + p + 1], (E, LANES)) for j in range(3)]
        for t in range(plan.tiles):
            def at(i):
                return masses[i * E:(i + 1) * E, t * LANES:(t + 1) * LANES]

            def slope(pos, step):
                if pos == 0:
                    return at(p + step) - at(p)
                if pos == 1:
                    return 0.5 * (at(p + step) - at(p - step))
                return at(p) - at(p - step)

            value = at(p) - (w[0] * at(p) + w[1] * slope(p % 3, 1) + w[2] * slope(p // 3, 3))
            out_ref[t, pl.ds(p, E, stride=9), :] = value


def listed_kernel(plan, count, tab_ref, own_ref, y_ref):
    ids = table_block(plan, tab_ref, "y", count)[:, GROUP - 1:GROUP]
    high, low = in_slots(plan, plan.unpack(own_ref), ids)
    listed = high + low
    plan.pack(lambda t: listed[:, t * LANES:(t + 1) * LANES], ((y_ref, table_for(plan, tab_ref, "y", count)),))


def own_kernel(plan, own_ref, mat_ref, acc_ref):
    acc_ref[...] = product(plan, mat_ref[0], *split(plan.unpack(own_ref)))


def reorder(plan, ref, out_ref):
    ids = group_table(plan, ref, 1)[:, GROUP - 1:GROUP]
    high, low = in_slots(plan, plan.unpack(ref), ids)
    listed = high + low
    table = ref[plan.table:plan.table + plan.slots, :]
    plan.pack(lambda t: listed[:, t * LANES:(t + 1) * LANES], ((out_ref, table),))


def shared_kernel(plan, x_ref, out_ref):
    reorder(plan, x_ref, out_ref)


def pick_kernel(plan, count, w_ref, x_ref, out_ref):
    index = lax.axis_index("curve")
    beside = (index == 1) | (index == count - 2)
    pl.when(beside)(lambda: reorder(plan, w_ref, out_ref))

    @pl.when(jnp.logical_not(beside))
    def _():
        out_ref[...] = x_ref[...]


def all_at_once():
    return lax.axis_index("curve") == 0


def next_kernel(plan, count, name, in_acc_ref, in_w_ref, hot_ref, mat_ref, *refs):
    acc_ref, w_ref = refs[-2:]

    def work_off(names):
        acc, weights = in_acc_ref[...], in_w_ref[0:plan.elements, :]
        for each, ref in zip(names, refs):
            more, extra = arrived(plan, each, count, ref, hot_ref, mat_ref)
            acc, weights = acc + more, weights + extra
        acc_ref[...] = acc
        w_ref[...] = weights

    if name == "w":
        return work_off("w")
    pl.when(jnp.logical_not(all_at_once()))(lambda: work_off(name))

    @pl.when(all_at_once())
    def _():
        if name == "x":
            work_off("xy")
        else:
            acc_ref[...] = in_acc_ref[...]
            w_ref[...] = in_w_ref[...]


def last_kernel(plan, count, acc_ref, in_w_ref, hot_ref, mat_ref, own_ref, f_ref, y_ref, out_ref, t_ref):
    def work_off(names):
        inflow, weights = acc_ref[...], in_w_ref[...]
        for name in names:
            more, extra = arrived(plan, name, count, f_ref if name == "f" else y_ref, hot_ref, mat_ref)
            inflow, weights = inflow + more, weights + extra
        kept(plan, plan.unpack(own_ref), weights, t_ref)
        for t in range(plan.full):
            out_ref[:, t * LANES:(t + 1) * LANES] = t_ref[t] + inflow[:, t * LANES:(t + 1) * LANES]
        if plan.rest:
            at = plan.full * LANES
            out_ref[:, at:plan.width] = (t_ref[plan.full] + inflow[:, at:at + LANES])[:, :plan.rest]

    pl.when(all_at_once())(lambda: work_off("f"))
    pl.when(jnp.logical_not(all_at_once()))(lambda: work_off("y"))


GRANT = pltpu.CompilerParams(vmem_limit_bytes=8 * 2**20)
VMEM = pl.BlockSpec(memory_space=pltpu.VMEM)
SMEM = pl.BlockSpec(memory_space=pltpu.SMEM)


HBM = pl.BlockSpec(memory_space=pltpu.HBM)


def far(*arrays):
    return [pltpu.with_memory_space_constraint(a, pltpu.HBM) for a in arrays]


def near(*arrays):
    return [pltpu.with_memory_space_constraint(a, pltpu.VMEM) for a in arrays]


def local(tracer_mass, send_ids, send_counts, sources, fractions, moments):
    count = lax.axis_size("curve")
    cells, width = tracer_mass.shape
    slots = send_ids.shape[1]
    elements = cells // 9
    plan = Plan(cells, width, elements, slots)
    src, fr, mo = sources.T, fractions.T, jnp.transpose(moments, (0, 2, 1))
    payload_t = pltpu.VMEM((plan.rows, LANES), F32)
    masses_t = pltpu.VMEM((cells, plan.lanes), F32)
    weights_t = pltpu.VMEM((elements, LANES), F32)
    work_t = pltpu.VMEM((plan.tiles, cells, LANES), F32)
    pay_x, pay_w, table, hot, *pieces = pl.pallas_call(
        functools.partial(pack_kernel, plan, count),
        out_shape=(
            payload_t,
            payload_t,
            pltpu.VMEM((elements + 4 * slots, LANES), F32),
            pltpu.VMEM((4, elements, slots), BF16),
            pltpu.VMEM(src.shape, jnp.int32),
            pltpu.VMEM(fr.shape, F32),
            pltpu.VMEM(mo.shape, F32),
        ),
        in_specs=[HBM] * 6,
        out_specs=(VMEM,) * 7,
        scratch_shapes=[
            pltpu.VMEM(tracer_mass.shape, F32),
            pltpu.VMEM(send_ids.shape, jnp.int32),
            pltpu.SMEM(send_counts.shape, jnp.int32),
            work_t,
            pltpu.SemaphoreType.DMA((6,)),
        ],
        compiler_params=GRANT,
        name="pack",
    )(*far(tracer_mass, src, fr, mo, send_ids, send_counts))

    def steps(by):
        pairs = [(i, i + (by if i % 2 else -by)) for i in range(count)]
        inside = [(i, j if 0 <= j < count else i ^ 1) for i, j in pairs]
        return inside, [(i, j % count) for i, j in pairs if not 0 <= j < count]

    towards, closing_x = steps(2)
    away, closing_y = steps(-2)
    swap = [(i, i ^ 1) for i in range(count)]
    closing = dict(closing_x + closing_y)
    closing = [(i, closing.get(i, i ^ 1)) for i in range(count)]
    got_x = lax.ppermute(pay_x, "curve", towards)
    got_w = lax.ppermute(pay_w, "curve", closing)
    cost = pl.CostEstimate(flops=10**9, bytes_accessed=10**6, transcendentals=0)
    matrix = pl.pallas_call(
        functools.partial(matrix_kernel, plan),
        out_shape=pltpu.VMEM((5, cells, 16 * elements + LANES), BF16),
        in_specs=[VMEM] * 3,
        out_specs=VMEM,
        scratch_shapes=[pltpu.VMEM((cells, LANES), F32)],
        cost_estimate=cost,
        compiler_params=GRANT,
        name="matrix",
    )(*near(*pieces))
    pay_y = pl.pallas_call(
        functools.partial(listed_kernel, plan, count),
        out_shape=payload_t,
        in_specs=[VMEM] * 2,
        out_specs=VMEM,
        cost_estimate=cost,
        compiler_params=GRANT,
        name="listed",
    )(*near(table, pay_x))
    acc = pl.pallas_call(
        functools.partial(own_kernel, plan),
        out_shape=masses_t,
        in_specs=[VMEM] * 2,
        out_specs=VMEM,
        cost_estimate=cost,
        compiler_params=GRANT,
        name="own",
    )(*near(pay_x, matrix))
    got_y = lax.ppermute(pay_y, "curve", away)
    got_s = lax.ppermute(pay_y, "curve", swap)
    shared = pl.pallas_call(
        functools.partial(shared_kernel, plan),
        out_shape=payload_t,
        in_specs=[VMEM],
        out_specs=VMEM,
        cost_estimate=cost,
        compiler_params=GRANT,
        name="shared",
    )(*near(got_x))
    shared = pl.pallas_call(
        functools.partial(pick_kernel, plan, count),
        out_shape=payload_t,
        in_specs=[VMEM] * 2,
        out_specs=VMEM,
        cost_estimate=cost,
        compiler_params=GRANT,
        name="pick",
    )(*near(got_w, shared))
    got_f = lax.ppermute(shared, "curve", swap)
    weights = table
    for name, blocks in (("x", (got_x, got_s)), ("w", (got_w,)), ("f", (got_f,))):
        acc, weights = pl.pallas_call(
            functools.partial(next_kernel, plan, count, name),
            out_shape=(masses_t, weights_t),
            in_specs=[VMEM] * (4 + len(blocks)),
            out_specs=(VMEM, VMEM),
            input_output_aliases={0: 0},
            cost_estimate=cost,
            compiler_params=GRANT,
        )(*near(acc, weights, hot, matrix, *blocks))
    return pl.pallas_call(
        functools.partial(last_kernel, plan, count),
        out_shape=jax.ShapeDtypeStruct((cells, width), F32),
        in_specs=[VMEM] * 7,
        out_specs=VMEM,
        scratch_shapes=[work_t],
        compiler_params=GRANT,
        name="last",
    )(*near(acc, weights, hot, matrix, pay_x, got_f, got_y))


def solution(mesh):
    placed = (
        P(("groups", "curve"), None),
        P(("groups", "curve"), None),
        P(("groups", "curve")),
        P(("groups", "curve"), None),
        P(("groups", "curve"), None),
        P(None, ("groups", "curve"), None),
    )
    return jax.shard_map(
        local, mesh=mesh, in_specs=placed, out_specs=P(("groups", "curve"), None), check_vma=False
    )
```

```python
import functools

import jax
import jax.numpy as jnp
from jax import lax
from jax.experimental import pallas as pl
from jax.experimental.pallas import tpu as pltpu
from jax.sharding import PartitionSpec as P


LANES = 128
F32 = jnp.float32
BF16 = jnp.bfloat16
GROUP = 28


def round8(n):
    return -(-n // 8) * 8


class Plan:
    def __init__(self, cells, width, elements, slots):
        self.cells, self.width, self.elements, self.slots = cells, width, elements, slots
        self.full = width // LANES
        rest = width % LANES
        self.rest = rest
        self.parts = []
        row = self.full * cells
        lane, size = 0, LANES // 2
        self.table = None
        while rest:
            if rest >= size:
                height = round8(-(-cells * size // LANES))
                if rest == size and height <= slots and -(-cells // slots) * size + 2 * GROUP <= LANES:
                    height, self.table, self.base = slots, row, -(-cells // slots) * size
                self.parts.append((lane, size, height, row))
                row += height
                lane += size
                rest -= size
            size //= 2
        if self.table is None:
            self.table, self.base = row, 0
            row += slots
        self.rows = row
        self.tiles = self.full + (1 if self.parts else 0)
        self.lanes = self.tiles * LANES

    def pack(self, tile_rows, outs):
        cells = self.cells
        lanes = lax.broadcasted_iota(jnp.int32, (1, LANES), 1)
        for t in range(self.full):
            tile = tile_rows(t)
            for out, _ in outs:
                out[t * cells:(t + 1) * cells, :] = tile
        if self.parts:
            last = tile_rows(self.full)
        for lane, size, height, first in self.parts:
            total = None
            for g in range(-(-cells // height)):
                count = min(height, cells - g * height)
                piece = last[g * height:g * height + count]
                shift = (g * size - lane) % LANES
                if shift:
                    piece = pltpu.roll(piece, shift, 1)
                if count < height:
                    piece = jnp.concatenate([piece, jnp.zeros((height - count, LANES), F32)], axis=0)
                total = piece if total is None else jnp.where(lanes >= g * size, piece, total)
            for out, table in outs:
                both = jnp.where(lanes >= self.base, table, total) if first == self.table else total
                out[first:first + height, :] = both
        if all(first != self.table for _, _, _, first in self.parts):
            for out, table in outs:
                out[self.table:self.rows, :] = table

    def unpack(self, ref):
        cells = self.cells
        tiles = [ref[t * cells:(t + 1) * cells, :] for t in range(self.full)]
        lanes = lax.broadcasted_iota(jnp.int32, (1, LANES), 1)
        if self.parts:
            last = None
            for lane, size, height, first in self.parts:
                block = ref[first:first + height, :]
                pieces = []
                for g in range(-(-cells // height)):
                    shift = (lane - g * size) % LANES
                    piece = pltpu.roll(block, shift, 1) if shift else block
                    pieces.append(piece[:min(height, cells - g * height)])
                piece = jnp.concatenate(pieces, axis=0)
                last = piece if last is None else jnp.where(lanes >= lane, piece, last)
            tiles.append(last)
        return jnp.concatenate(tiles, axis=1)


def split(x):
    high = x.astype(BF16)
    return high, (x - high.astype(F32)).astype(BF16)


def dot(a, b):
    return jnp.dot(a, b, preferred_element_type=F32)


def element_and_place(src):
    elem = ((src.astype(F32) + 0.5) * (1.0 / 9.0)).astype(jnp.int32)
    return elem, src - 9 * elem


def sent_list(name, count):
    index = lax.axis_index("curve")
    odd = lax.rem(index, 2) == 1
    end = (index == 0) | (index == count - 1)
    beside = (index == 1) | (index == count - 2)
    swap = jnp.where(odd, 2, 0)
    near = jnp.where(odd, 1, 3)
    far = jnp.where(odd, 3, 1)
    if name == "f":
        return jnp.where(odd, 0, 2)
    if name == "w":
        return jnp.where(end, near, jnp.where(beside, far, swap))
    if name == "x":
        return jnp.where(end, swap, near)
    return jnp.where(beside, swap, far)


def table_block(plan, tab_ref, name, count):
    at = plan.elements + plan.slots * lax.rem(sent_list(name, count) + 2, 4)
    return tab_ref[pl.ds(pl.multiple_of(at, 8), plan.slots), :]


def table_for(plan, tab_ref, name, count):
    lanes = lax.broadcasted_iota(jnp.int32, (1, LANES), 1)
    one = table_block(plan, tab_ref, name, count)
    one = pltpu.roll(one, plan.base, 1) if plan.base else one
    two = pltpu.roll(table_block(plan, tab_ref, "f", count), plan.base + GROUP, 1)
    return jnp.where(lanes >= plan.base + GROUP, two, one)


def pack_kernel(plan, count, q_hbm, src_hbm, fr_hbm, mo_hbm, ids_hbm, cnt_hbm,
                x_ref, w_ref, tab_ref, hot_ref, src_ref, fr_ref, mo_ref,
                q_ref, ids_ref, cnt_ref, t_ref, sems):
    E = plan.elements
    copies = [
        pltpu.make_async_copy(a, b, sems.at[n])
        for n, (a, b) in enumerate((
            (src_hbm, src_ref), (fr_hbm, fr_ref), (mo_hbm, mo_ref),
            (cnt_hbm, cnt_ref), (ids_hbm, ids_ref), (q_hbm, q_ref),
        ))
    ]
    for copy in copies:
        copy.start()
    for copy in copies[:5]:
        copy.wait()
    weights_table(plan, src_ref, fr_ref, mo_ref, ids_ref, cnt_ref, tab_ref)
    copies[5].wait()
    for t in range(plan.full):
        t_ref[t] = q_ref[:, t * LANES:(t + 1) * LANES]
    if plan.rest:
        t_ref[plan.full, :, 0:plan.rest] = q_ref[:, plan.full * LANES:plan.width]

    def tile_rows(t):
        return jnp.concatenate([t_ref[t, pl.ds(p, E, stride=9), :] for p in range(9)], axis=0)

    tables = [table_for(plan, tab_ref, name, count) for name in "xw"]
    plan.pack(tile_rows, ((x_ref, tables[0]), (w_ref, tables[1])))
    for n, name in enumerate("wxyf"):
        hot_ref[n] = live_slots(plan, my_list(name, count), ids_ref, cnt_ref)


def weights_table(plan, src_ref, fr_ref, mo_ref, ids_ref, cnt_ref, tab_ref):
    cells, E, S = plan.cells, plan.elements, plan.slots
    elem, place = element_and_place(src_ref[...])
    fr = fr_ref[...]
    wx = fr * mo_ref[0]
    wy = fr * mo_ref[1]
    total = E + 4 * S
    pieces = src_ref.shape[0]
    main = cells // LANES * LANES

    def flat(x):
        rows = [x[k:k + 1, :main] for k in range(pieces)]
        return jnp.concatenate(rows + [x[k:k + 1, main:] for k in range(pieces)], axis=1)

    elem, place, fr, wx, wy = (flat(x) for x in (elem, place, fr, wx, wy))
    many = pieces * cells
    erow = lax.broadcasted_iota(jnp.int32, (total, many), 0)
    urow = lax.broadcasted_iota(jnp.int32, (32, many), 0)
    uplace = urow - jnp.where(urow < 9, 0, jnp.where(urow < 18, 9, 18))
    hot = jnp.where(erow == elem, 1.0, 0.0).astype(BF16)
    value = jnp.where(urow < 9, fr, jnp.where(urow < 18, wx, wy))
    high, low = split(jnp.where(uplace == place, value, 0.0))
    both = jnp.concatenate([high, low, jnp.zeros((64, many), BF16)], axis=0)
    acc = lax.dot_general(hot, both, (((1,), (1,)), ((), ())), preferred_element_type=F32)
    acc = acc + pltpu.roll(acc, LANES - 32, 1)
    tab_ref[0:E, :] = acc[0:E]
    lane = lax.broadcasted_iota(jnp.int32, (1, LANES), 1)
    diag = lax.broadcasted_iota(jnp.int32, (S, S), 0) == lax.broadcasted_iota(jnp.int32, (S, S), 1)
    slot = lax.broadcasted_iota(jnp.int32, (1, S), 1)
    for o in range(4):
        sent = (o + 2) % 4
        ids = jnp.where(slot < cnt_ref[sent], ids_ref[sent:sent + 1, :].astype(F32), -1.0)
        column = jnp.sum(jnp.where(diag, ids, 0.0), axis=1, keepdims=True)
        part = acc[E + o * S:E + (o + 1) * S]
        tab_ref[E + o * S:E + (o + 1) * S, :] = jnp.where(lane == GROUP - 1, column, part)


def matrix_kernel(plan, src_ref, fr_ref, mo_ref, mat_ref, col_ref):
    cells, E = plan.cells, plan.elements
    K = src_ref.shape[0]
    elem, place = element_and_place(src_ref[...])
    fr = fr_ref[...]
    wx = fr * mo_ref[0]
    wy = fr * mo_ref[1]
    row = jnp.where(place >= 6, 2, jnp.where(place >= 3, 1, 0))
    r = row.astype(F32)
    c = (place - 3 * row).astype(F32)
    centre = fr + wx * (c - 1.0) + wy * (r - 1.0)
    rows = [
        elem.astype(F32), place.astype(F32), centre,
        wx * (1.0 - 0.5 * c), wx * (-0.5 * c), wy * (1.0 - 0.5 * r), wy * (-0.5 * r),
    ]
    rows = jnp.concatenate(rows + [jnp.zeros((LANES - 7 * K, cells), F32)], axis=0)
    pad = -cells % LANES
    if pad:
        rows = jnp.concatenate([rows, jnp.zeros((LANES, pad), F32)], axis=1)
    col_ref[...] = jnp.transpose(rows, (1, 0))[0:cells]
    step = E
    lane = lax.broadcasted_iota(jnp.int32, (step, LANES), 1)
    per = LANES // E
    lists = mat_ref.shape[0]
    main = 8 * E

    def body(i, carry):
        at = pl.multiple_of(i * step, step)
        cols = col_ref[pl.ds(at, step), :]

        def wide(n, k):
            return jnp.broadcast_to(cols[:, n * K + k:n * K + k + 1], (step, LANES))

        inner = (lane % E).astype(F32)
        for t in range(main // LANES + 1):
            tail = t == main // LANES
            where = jnp.full((step, LANES), 8.0) if tail else (lane // E + per * t).astype(F32)
            sums = [jnp.zeros((step, LANES), F32) for _ in range(lists)]
            for k in range(K):
                d = where - wide(1, k)
                coef = jnp.where(d == 0.0, wide(2, k), 0.0)
                coef = jnp.where(d == 1.0, wide(3, k), coef)
                coef = jnp.where(d == 3.0, wide(5, k), coef)
                if not tail:
                    coef = jnp.where(d == -1.0, wide(4, k), coef)
                    coef = jnp.where(d == -3.0, wide(6, k), coef)
                e = wide(0, k) - inner
                for n in range(lists):
                    sums[n] = sums[n] + jnp.where(e == float(n * E), coef, 0.0)
            for n in range(lists):
                high, low = split(sums[n])
                if tail:
                    both = jnp.where(lane < 2 * E, high.astype(F32), low.astype(F32)).astype(BF16)
                    mat_ref[n, pl.ds(at, step), 2 * main:2 * main + LANES] = both
                else:
                    mat_ref[n, pl.ds(at, step), t * LANES:(t + 1) * LANES] = high
                    mat_ref[n, pl.ds(at, step), main + t * LANES:main + (t + 1) * LANES] = low
        return carry

    lax.fori_loop(0, cells // step, body, 0)


def in_slots(plan, masses, ids):
    E = plan.elements
    high, low = split(masses)
    per = LANES // E
    r = lax.broadcasted_iota(jnp.int32, (LANES, LANES), 0)
    l = lax.broadcasted_iota(jnp.int32, (LANES, LANES), 1)
    many = jnp.concatenate([ids] * per, axis=0)
    hot = jnp.where(((l % E).astype(F32) == many) & (r // E == l // E), 1.0, 0.0).astype(BF16)
    pair = jnp.concatenate([high, low], axis=1)
    pieces = []
    for first in range(0, plan.cells, LANES):
        size = min(LANES, plan.cells - first)
        pieces.append(dot(hot[:size, :size], pair[first:first + size]))
    pair = jnp.concatenate(pieces, axis=0)
    return pair[:, :plan.lanes], pair[:, plan.lanes:]


def product(plan, mat, high, low):
    E = plan.elements
    main = 8 * E
    ends = jnp.concatenate([high[main:], low[main:], high[main:]], axis=0)
    return (
        dot(mat[:, :main], high[:main]) + dot(mat[:, :main], low[:main])
        + dot(mat[:, main:2 * main], high[:main]) + dot(mat[:, 2 * main:2 * main + 3 * E], ends)
    )


def group_table(plan, block, group):
    at = plan.base + GROUP * group
    table = block[plan.table:plan.table + plan.slots, :]
    return pltpu.roll(table, LANES - at, 1) if at else table


def returned_weights(table, hot):
    lane = lax.broadcasted_iota(jnp.int32, table.shape, 1)
    high, low = split(jnp.where(lane < GROUP - 1, table, 0.0))
    return dot(hot, high) + dot(hot, low)


def live_slots(plan, which, ids_ref, cnt_ref):
    E, S = plan.elements, plan.slots
    slot = lax.broadcasted_iota(jnp.int32, (E, S), 1)
    e = lax.broadcasted_iota(jnp.int32, (E, S), 0)
    live = (e == ids_ref[pl.ds(which, 1), :]) & (slot < cnt_ref[which])
    return jnp.where(live, 1.0, 0.0).astype(BF16)


def my_list(name, count):
    index = lax.axis_index("curve")
    odd = lax.rem(index, 2) == 1
    end = (index == 0) | (index == count - 1)
    beside = (index == 1) | (index == count - 2)
    swap = jnp.where(odd, 2, 0)
    near = jnp.where(odd, 3, 1)
    far = jnp.where(odd, 1, 3)
    if name == "f":
        return jnp.where(odd, 0, 2)
    if name == "w":
        return jnp.where(end, far, jnp.where(beside, near, swap))
    if name == "x":
        return jnp.where(beside, swap, near)
    return jnp.where(end, swap, far)


def arrived(plan, name, count, block, hot_ref, mat_ref):
    theirs = lax.rem(my_list(name, count) + 2, 4)
    table = group_table(plan, block, 1 if name == "f" else 0)
    weights = returned_weights(table, hot_ref["wxyf".index(name)])
    masses = plan.unpack(block)
    if name in "fy":
        high, low = split(masses)
    else:
        high, low = in_slots(plan, masses, table[:, GROUP - 1:GROUP])
        high, low = high.astype(BF16), low.astype(BF16)
    return product(plan, mat_ref[theirs + 1], high, low), weights


def kept(plan, masses, weights, out_ref):
    E = plan.elements
    for p in range(9):
        w = [jnp.broadcast_to(weights[:, 9 * j + p:9 * j + p + 1], (E, LANES)) for j in range(3)]
        for t in range(plan.tiles):
            def at(i):
                return masses[i * E:(i + 1) * E, t * LANES:(t + 1) * LANES]

            def slope(pos, step):
                if pos == 0:
                    return at(p + step) - at(p)
                if pos == 1:
                    return 0.5 * (at(p + step) - at(p - step))
                return at(p) - at(p - step)

            value = at(p) - (w[0] * at(p) + w[1] * slope(p % 3, 1) + w[2] * slope(p // 3, 3))
            out_ref[t, pl.ds(p, E, stride=9), :] = value


def listed_kernel(plan, count, tab_ref, own_ref, y_ref):
    ids = table_block(plan, tab_ref, "y", count)[:, GROUP - 1:GROUP]
    high, low = in_slots(plan, plan.unpack(own_ref), ids)
    listed = high + low
    plan.pack(lambda t: listed[:, t * LANES:(t + 1) * LANES], ((y_ref, table_for(plan, tab_ref, "y", count)),))


def own_kernel(plan, own_ref, mat_ref, acc_ref, masses_ref):
    masses = plan.unpack(own_ref)
    masses_ref[...] = masses
    acc_ref[...] = product(plan, mat_ref[0], *split(masses))


def reorder(plan, ref, out_ref):
    ids = group_table(plan, ref, 1)[:, GROUP - 1:GROUP]
    high, low = in_slots(plan, plan.unpack(ref), ids)
    listed = high + low
    table = ref[plan.table:plan.table + plan.slots, :]
    plan.pack(lambda t: listed[:, t * LANES:(t + 1) * LANES], ((out_ref, table),))


def shared_kernel(plan, x_ref, out_ref):
    reorder(plan, x_ref, out_ref)


def pick_kernel(plan, count, w_ref, x_ref, out_ref):
    index = lax.axis_index("curve")
    beside = (index == 1) | (index == count - 2)
    pl.when(beside)(lambda: reorder(plan, w_ref, out_ref))

    @pl.when(jnp.logical_not(beside))
    def _():
        out_ref[...] = x_ref[...]


def all_at_once():
    return lax.axis_index("curve") == 0


def next_kernel(plan, count, name, in_acc_ref, in_w_ref, hot_ref, mat_ref, ref, acc_ref, w_ref):
    def work_off():
        acc, weights = in_acc_ref[...], in_w_ref[0:plan.elements, :]
        more, extra = arrived(plan, name, count, ref, hot_ref, mat_ref)
        acc_ref[...] = acc + more
        w_ref[...] = weights + extra

    if name != "f":
        return work_off()
    pl.when(jnp.logical_not(all_at_once()))(work_off)

    @pl.when(all_at_once())
    def _():
        acc_ref[...] = in_acc_ref[...]
        w_ref[...] = in_w_ref[...]


def last_kernel(plan, count, acc_ref, in_w_ref, hot_ref, mat_ref, own_ref, f_ref, y_ref, out_ref, t_ref):
    def work_off(names):
        inflow, weights = acc_ref[...], in_w_ref[...]
        for name in names:
            more, extra = arrived(plan, name, count, f_ref if name == "f" else y_ref, hot_ref, mat_ref)
            inflow, weights = inflow + more, weights + extra
        kept(plan, own_ref[...], weights, t_ref)
        for t in range(plan.full):
            out_ref[:, t * LANES:(t + 1) * LANES] = t_ref[t] + inflow[:, t * LANES:(t + 1) * LANES]
        if plan.rest:
            at = plan.full * LANES
            out_ref[:, at:plan.width] = (t_ref[plan.full] + inflow[:, at:at + LANES])[:, :plan.rest]

    pl.when(all_at_once())(lambda: work_off("fy"))
    pl.when(jnp.logical_not(all_at_once()))(lambda: work_off("y"))


GRANT = pltpu.CompilerParams(vmem_limit_bytes=8 * 2**20)
VMEM = pl.BlockSpec(memory_space=pltpu.VMEM)
SMEM = pl.BlockSpec(memory_space=pltpu.SMEM)


HBM = pl.BlockSpec(memory_space=pltpu.HBM)


def far(*arrays):
    return [pltpu.with_memory_space_constraint(a, pltpu.HBM) for a in arrays]


def near(*arrays):
    return [pltpu.with_memory_space_constraint(a, pltpu.VMEM) for a in arrays]


def local(tracer_mass, send_ids, send_counts, sources, fractions, moments):
    count = lax.axis_size("curve")
    cells, width = tracer_mass.shape
    slots = send_ids.shape[1]
    elements = cells // 9
    plan = Plan(cells, width, elements, slots)
    src, fr, mo = sources.T, fractions.T, jnp.transpose(moments, (0, 2, 1))
    payload_t = pltpu.VMEM((plan.rows, LANES), F32)
    masses_t = pltpu.VMEM((cells, plan.lanes), F32)
    weights_t = pltpu.VMEM((elements, LANES), F32)
    work_t = pltpu.VMEM((plan.tiles, cells, LANES), F32)
    pay_x, pay_w, table, hot, *pieces = pl.pallas_call(
        functools.partial(pack_kernel, plan, count),
        out_shape=(
            payload_t,
            payload_t,
            pltpu.VMEM((elements + 4 * slots, LANES), F32),
            pltpu.VMEM((4, elements, slots), BF16),
            pltpu.VMEM(src.shape, jnp.int32),
            pltpu.VMEM(fr.shape, F32),
            pltpu.VMEM(mo.shape, F32),
        ),
        in_specs=[HBM] * 6,
        out_specs=(VMEM,) * 7,
        scratch_shapes=[
            pltpu.VMEM(tracer_mass.shape, F32),
            pltpu.VMEM(send_ids.shape, jnp.int32),
            pltpu.SMEM(send_counts.shape, jnp.int32),
            work_t,
            pltpu.SemaphoreType.DMA((6,)),
        ],
        compiler_params=GRANT,
        name="pack",
    )(*far(tracer_mass, src, fr, mo, send_ids, send_counts))

    def steps(by):
        pairs = [(i, i + (by if i % 2 else -by)) for i in range(count)]
        inside = [(i, j if 0 <= j < count else i ^ 1) for i, j in pairs]
        return inside, [(i, j % count) for i, j in pairs if not 0 <= j < count]

    towards, closing_x = steps(2)
    away, closing_y = steps(-2)
    swap = [(i, i ^ 1) for i in range(count)]
    closing = dict(closing_x + closing_y)
    closing = [(i, closing.get(i, i ^ 1)) for i in range(count)]
    got_x = lax.ppermute(pay_x, "curve", towards)
    got_w = lax.ppermute(pay_w, "curve", closing)
    cost = pl.CostEstimate(flops=10**9, bytes_accessed=10**6, transcendentals=0)
    matrix = pl.pallas_call(
        functools.partial(matrix_kernel, plan),
        out_shape=pltpu.VMEM((5, cells, 16 * elements + LANES), BF16),
        in_specs=[VMEM] * 3,
        out_specs=VMEM,
        scratch_shapes=[pltpu.VMEM((cells, LANES), F32)],
        cost_estimate=cost,
        compiler_params=GRANT,
        name="matrix",
    )(*near(*pieces))
    pay_y = pl.pallas_call(
        functools.partial(listed_kernel, plan, count),
        out_shape=payload_t,
        in_specs=[VMEM] * 2,
        out_specs=VMEM,
        cost_estimate=cost,
        compiler_params=GRANT,
        name="listed",
    )(*near(table, pay_x))
    acc, masses = pl.pallas_call(
        functools.partial(own_kernel, plan),
        out_shape=(masses_t, masses_t),
        in_specs=[VMEM] * 2,
        out_specs=(VMEM, VMEM),
        cost_estimate=cost,
        compiler_params=GRANT,
        name="own",
    )(*near(pay_x, matrix))
    got_y = lax.ppermute(pay_y, "curve", away)
    shared = pl.pallas_call(
        functools.partial(shared_kernel, plan),
        out_shape=payload_t,
        in_specs=[VMEM],
        out_specs=VMEM,
        cost_estimate=cost,
        compiler_params=GRANT,
        name="shared",
    )(*near(got_x))
    shared = pl.pallas_call(
        functools.partial(pick_kernel, plan, count),
        out_shape=payload_t,
        in_specs=[VMEM] * 2,
        out_specs=VMEM,
        cost_estimate=cost,
        compiler_params=GRANT,
        name="pick",
    )(*near(got_w, shared))
    got_f = lax.ppermute(shared, "curve", swap)
    weights = table
    for name, block in (("x", got_x), ("w", got_w), ("f", got_f)):
        acc, weights = pl.pallas_call(
            functools.partial(next_kernel, plan, count, name),
            out_shape=(masses_t, weights_t),
            in_specs=[VMEM] * 5,
            out_specs=(VMEM, VMEM),
            input_output_aliases={0: 0},
            cost_estimate=cost,
            compiler_params=GRANT,
        )(*near(acc, weights, hot, matrix, block))
    return pl.pallas_call(
        functools.partial(last_kernel, plan, count),
        out_shape=jax.ShapeDtypeStruct((cells, width), F32),
        in_specs=[VMEM] * 7,
        out_specs=VMEM,
        scratch_shapes=[work_t],
        compiler_params=GRANT,
        name="last",
    )(*near(acc, weights, hot, matrix, masses, got_f, got_y))


def solution(mesh):
    placed = (
        P(("groups", "curve"), None),
        P(("groups", "curve"), None),
        P(("groups", "curve")),
        P(("groups", "curve"), None),
        P(("groups", "curve"), None),
        P(None, ("groups", "curve"), None),
    )
    return jax.shard_map(
        local, mesh=mesh, in_specs=placed, out_specs=P(("groups", "curve"), None), check_vma=False
    )
```
